32 devices in a mesh: dp: 2 (over x), y: 4 (over z), x: 4 (over y, core).
Axes of the slice: x: 2, y: 2, z: 4, core: 2. Of those that a mesh axis runs over, the one named last changes fastest.
Arguments:
- tokens: int32 [3, 512], P(None, 'dp'), parts along dimension 1
- lengths: int32 [512], P('dp'), parts along dimension 0
- choices: int32 [3, 512, 8], P(None, 'dp'), parts along dimension 1
- emb_table: bfloat16 [49152, 1536], P(None, 'x')
- k_cache: bfloat16 [512, 256, 8, 64], P('dp', None, 'y'), parts along dimension 0
- v_cache: bfloat16 [512, 256, 8, 64], P('dp', None, 'y'), parts along dimension 0
- g_attn: bfloat16 [1536], P('x')
- w_q: bfloat16 [1536, 1536], P('x', 'y')
- w_k: bfloat16 [1536, 512], P('x', 'y')
- w_v: bfloat16 [1536, 512], P('x', 'y')
- w_o: bfloat16 [1536, 1536], P('y', 'x')
- g_ffn: bfloat16 [1536], P('x')
- w_router: bfloat16 [1536, 40], P('x')
- w_act: bfloat16 [40, 1536, 512], P(None, 'x', 'y')
- w_lin: bfloat16 [40, 1536, 512], P(None, 'x', 'y')
- w_down: bfloat16 [40, 512, 1536], P(None, 'y', 'x')
Outputs:
- output 1: bfloat16 [3, 512, 1536], P(None, 'dp', 'x'), parts along dimension 1
- output 2: bfloat16 [512, 256, 8, 64], P('dp', None, 'y'), parts along dimension 0
- output 3: bfloat16 [512, 256, 8, 64], P('dp', None, 'y'), parts along dimension 0
There are 2 independent parts. The reference program is written for one: setup_inputs(seed, part) draws one part's arguments, and reference() takes and returns one part's arrays. A program takes and returns all parts, laid end to end along the dimension named above; an argument that names none is the same for every part.
All inputs are finite; a program needn't handle non-finite values.
Results may differ from the reference program's by a relative error of at most 0.0115555.
Values are sent between devices in bfloat16 or wider.
A program may use at most 1 GiB of HBM per device.

```python
import math
import jax
import jax.numpy as jnp
from jax import lax

BATCH = 256
SEQ = 256
D = 1536
HEADS = 24
KV_HEADS = 8
HEAD = 64
FF = 512
EXPERTS = 40
TOP = 8
VOCAB = 49152
STEPS = 3

EPS = 1e-5
ROPE_BASE = 1.0e6
LOG_SEQ = int(math.log2(SEQ))
HOT_COUNT = max(1, EXPERTS // 8)
GROUP_SIZE = HEADS // KV_HEADS


def draw_lengths(key_a, key_b, key_c):
    exponent = jax.random.randint(key_a, (BATCH,), 0, LOG_SEQ + 1)
    len_limit = jnp.minimum(jnp.left_shift(jnp.ones((BATCH,), jnp.int32), exponent), SEQ - 3)
    raw_draw = jax.random.randint(key_b, (BATCH,), 0, 1 << 30)
    lengths = 1 + raw_draw % len_limit
    pick_row = jax.random.randint(key_c, (), 0, BATCH)
    row_ids = jnp.arange(BATCH)
    lengths = jnp.where(row_ids == pick_row, SEQ - 3, lengths)
    lengths = jnp.where(row_ids == (pick_row + 1) % BATCH, 1, lengths)
    return lengths.astype(jnp.int32)


def draw_choices(key_a, key_b):
    expert_rank = jax.random.permutation(key_a, EXPERTS)
    hot_bonus = jnp.where(expert_rank < HOT_COUNT, EXPERTS, 0)
    noise_int = jax.random.randint(key_b, (STEPS, BATCH, EXPERTS), 0, 2 * EXPERTS)
    scores = (noise_int + hot_bonus) * EXPERTS + jnp.arange(EXPERTS)
    return lax.top_k(scores, TOP)[1].astype(jnp.int32)


def normal_weights(key_w, shape_w, scale_w):
    return (jax.random.normal(key_w, shape_w, jnp.float32) * scale_w).astype(jnp.bfloat16)


def setup_inputs(seed: int = 0, part: int = 0) -> dict:
    base_key = jax.random.key(seed)
    weight_keys = jax.random.split(base_key, 12)
    part_keys = jax.random.split(jax.random.fold_in(base_key, part), 8)
    tokens = jax.random.randint(part_keys[0], (STEPS, BATCH), 0, VOCAB)
    lengths = draw_lengths(part_keys[1], part_keys[2], part_keys[3])
    choices = draw_choices(part_keys[4], part_keys[5])
    k_cache = normal_weights(part_keys[6], (BATCH, SEQ, KV_HEADS, HEAD), 1.0)
    v_cache = normal_weights(part_keys[7], (BATCH, SEQ, KV_HEADS, HEAD), 1.0)
    ramp_rate = jax.random.uniform(weight_keys[0], (), jnp.float32, 0.6, 1.2)
    col_scale = jnp.exp(ramp_rate * jnp.linspace(-1.0, 1.0, D))
    emb_table = (jax.random.normal(weight_keys[1], (VOCAB, D), jnp.float32) * col_scale).astype(jnp.bfloat16)
    g_attn = (1.0 + 0.3 * jax.random.normal(weight_keys[2], (D,), jnp.float32)).astype(jnp.bfloat16)
    w_q = normal_weights(weight_keys[3], (D, HEADS * HEAD), D ** -0.5)
    w_k = normal_weights(weight_keys[4], (D, KV_HEADS * HEAD), D ** -0.5)
    w_v = normal_weights(weight_keys[5], (D, KV_HEADS * HEAD), D ** -0.5)
    w_o = normal_weights(weight_keys[6], (HEADS * HEAD, D), (HEADS * HEAD) ** -0.5)
    g_ffn = (1.0 + 0.3 * jax.random.normal(weight_keys[7], (D,), jnp.float32)).astype(jnp.bfloat16)
    w_router = normal_weights(weight_keys[8], (D, EXPERTS), 1.5 * D ** -0.5)
    w_act = normal_weights(weight_keys[9], (EXPERTS, D, FF), D ** -0.5)
    w_lin = normal_weights(weight_keys[10], (EXPERTS, D, FF), D ** -0.5)
    w_down = normal_weights(weight_keys[11], (EXPERTS, FF, D), FF ** -0.5)
    return dict(tokens=tokens, lengths=lengths, choices=choices, emb_table=emb_table, k_cache=k_cache, v_cache=v_cache, g_attn=g_attn, w_q=w_q, w_k=w_k, w_v=w_v, w_o=w_o, g_ffn=g_ffn, w_router=w_router, w_act=w_act, w_lin=w_lin, w_down=w_down)


def rms_norm(x_val, gain_vec):
    x_f32 = x_val.astype(jnp.float32)
    meansq = jnp.sum(x_f32 * x_f32, axis=-1, keepdims=True) / D
    return (x_f32 * lax.rsqrt(meansq + EPS) * gain_vec.astype(jnp.float32)).astype(jnp.bfloat16)


def rotate(vectors, positions):
    half_dim = HEAD // 2
    inv_freq = ROPE_BASE ** (-(jnp.arange(half_dim).astype(jnp.float32) * 2.0 / HEAD))
    angles = positions.astype(jnp.float32)[:, None, None] * inv_freq
    cosine = jnp.cos(angles)
    sine_val = jnp.sin(angles)
    first_half = vectors[..., :half_dim].astype(jnp.float32)
    second_half = vectors[..., half_dim:].astype(jnp.float32)
    return jnp.concatenate([first_half * cosine - second_half * sine_val, second_half * cosine + first_half * sine_val], axis=-1).astype(jnp.bfloat16)


def attend_row(row_args):
    q_row, key_row, val_row, pos_row = row_args
    scores = jnp.einsum('kgh,skh->kgs', q_row.astype(jnp.float32), key_row.astype(jnp.float32)) * HEAD ** -0.5
    valid_mask = jnp.arange(SEQ) <= pos_row
    scores = jnp.where(valid_mask, scores, -1.0e30)
    peak_val = jnp.max(scores, axis=-1, keepdims=True)
    weight = jnp.where(valid_mask, jnp.exp(scores - peak_val), 0.0)
    total_w = jnp.sum(weight, axis=-1, keepdims=True)
    mixed_out = jnp.einsum('kgs,skh->kgh', weight.astype(jnp.bfloat16).astype(jnp.float32), val_row.astype(jnp.float32))
    return (mixed_out / total_w).astype(jnp.bfloat16)


def reference(tokens, lengths, choices, emb_table, k_cache, v_cache, g_attn, w_q, w_k, w_v, w_o, g_ffn, w_router, w_act, w_lin, w_down):
    slot_ids = jnp.arange(SEQ)
    expert_ids = jnp.arange(EXPERTS)

    def one_step(carry, step_in):
        key_cache, val_cache = carry
        tok_row, choice_row, step_idx = step_in
        positions = lengths + step_idx
        x_in = emb_table[tok_row]
        normed = rms_norm(x_in, g_attn)
        queries = rotate(jnp.dot(normed, w_q, preferred_element_type=jnp.float32).astype(jnp.bfloat16).reshape(BATCH, HEADS, HEAD), positions)
        new_keys = rotate(jnp.dot(normed, w_k, preferred_element_type=jnp.float32).astype(jnp.bfloat16).reshape(BATCH, KV_HEADS, HEAD), positions)
        new_vals = jnp.dot(normed, w_v, preferred_element_type=jnp.float32).astype(jnp.bfloat16).reshape(BATCH, KV_HEADS, HEAD)
        hit_mask = (slot_ids[None, :] == positions[:, None])[:, :, None, None]
        key_cache = jnp.where(hit_mask, new_keys[:, None], key_cache)
        val_cache = jnp.where(hit_mask, new_vals[:, None], val_cache)
        grouped = queries.reshape(BATCH, KV_HEADS, GROUP_SIZE, HEAD)
        mixed = lax.map(attend_row, (grouped, key_cache, val_cache, positions)).reshape(BATCH, HEADS * HEAD)
        x_mid = (x_in.astype(jnp.float32) + jnp.dot(mixed, w_o, preferred_element_type=jnp.float32)).astype(jnp.bfloat16)
        normed2 = rms_norm(x_mid, g_ffn)
        logits = jnp.dot(normed2, w_router, preferred_element_type=jnp.float32)
        gate_val = jax.nn.softmax(jnp.take_along_axis(logits, choice_row, axis=1), axis=-1)
        onehot = choice_row[:, :, None] == expert_ids[None, None, :]
        coef = jnp.sum(jnp.where(onehot, gate_val[:, :, None], 0.0), axis=1)

        def expert_out(expert_args):
            act_w, lin_w, down_w, coef_col = expert_args
            act_f32 = jnp.dot(normed2, act_w, preferred_element_type=jnp.float32)
            lin_f32 = jnp.dot(normed2, lin_w, preferred_element_type=jnp.float32)
            unit_bf16 = (coef_col[:, None] * jax.nn.silu(act_f32) * lin_f32).astype(jnp.bfloat16)
            return jnp.dot(unit_bf16, down_w, preferred_element_type=jnp.float32)

        moe_sum = jnp.sum(lax.map(expert_out, (w_act, w_lin, w_down, coef.T)), axis=0)
        hidden_out = (x_mid.astype(jnp.float32) + moe_sum).astype(jnp.bfloat16)
        return (key_cache, val_cache), hidden_out

    (k_out, v_out), hidden_out = lax.scan(one_step, (k_cache, v_cache), (tokens, choices, jnp.arange(STEPS)))
    return hidden_out, k_out, v_out
```

```python
import functools
import jax
import jax.numpy as jnp
from jax import lax
from jax.experimental import pallas as pl
from jax.experimental.pallas import tpu as pltpu
from jax.sharding import PartitionSpec as P

EPS = 1e-5
ROPE_BASE = 1.0e6
MESH = pl.DeviceIdType.MESH
F32 = jnp.float32
BF16 = jnp.bfloat16
NB = 8
QROWS = 16


def attn_body(len_ref, q_ref, kn_ref, vn_ref, k_ref, v_ref, o_ref, ko_ref, vo_ref, *, steps, group):
    seq = k_ref.shape[2]
    step = pl.program_id(0)
    knt = kn_ref[0].astype(F32).T.astype(BF16)
    vnt = vn_ref[0].astype(F32).T.astype(BF16)
    new_t = jnp.concatenate([knt, vnt], axis=0)
    n_new = new_t.shape[1]
    row_id = lax.broadcasted_iota(jnp.int32, (n_new, seq), 0)
    col_id = lax.broadcasted_iota(jnp.int32, (n_new, seq), 1)
    lane1 = lax.broadcasted_iota(jnp.int32, (1, seq), 1)
    srow = lax.broadcasted_iota(jnp.int32, (2 * QROWS, seq), 0)
    scol = lax.broadcasted_iota(jnp.int32, (2 * QROWS, seq), 1)
    srow = jnp.where(srow >= QROWS, srow - QROWS, srow)
    t_of = jnp.where(srow >= 2 * group, 2, jnp.where(srow >= group, 1, 0))
    rel = scol - t_of
    low = lax.broadcasted_iota(jnp.int32, (QROWS, 128), 1) < 64
    half = k_ref.shape[1]
    for b in range(NB):
        pos = len_ref[step * NB + b]
        place = jnp.where(row_id - b * steps == col_id - pos, 1.0, 0.0)
        place = jnp.where((row_id >= b * steps) & (row_id < (b + 1) * steps), place, 0.0).astype(BF16)
        placed = jnp.dot(new_t, place, preferred_element_type=F32).astype(BF16)
        hit = jnp.broadcast_to((lane1 >= pos) & (lane1 < pos + steps), (half, seq))
        k_new = jnp.where(hit, placed[:half], k_ref[b])
        v_new = jnp.where(hit, placed[half:], v_ref[b])
        ko_ref[b] = k_new
        vo_ref[b] = v_new
        q16 = q_ref[b]
        zero = jnp.zeros_like(q16)
        q32 = jnp.concatenate([jnp.where(low, q16, zero), jnp.where(low, zero, q16)], axis=0)
        s = jnp.dot(q32, k_new, preferred_element_type=F32) * 0.125
        ok = rel <= pos
        s = jnp.where(ok, s, -1.0e30)
        peak = jnp.max(s, axis=1, keepdims=True)
        w = jnp.where(ok, jnp.exp(s - peak), 0.0)
        tot = jnp.sum(w, axis=1, keepdims=True)
        o = lax.dot_general(w.astype(BF16), v_new, (((1,), (1,)), ((), ())), preferred_element_type=F32)
        o = o / tot
        o_ref[b] = jnp.where(low, o[:QROWS], o[QROWS:]).astype(BF16)


def attention(lengths, q, kn, vn, kc, vc, steps, group):
    nb, half, seq = kc.shape
    grid = nb // NB
    cache = pl.BlockSpec((NB, half, seq), lambda i, l: (i, 0, 0))
    new = pl.BlockSpec((1,) + kn.shape[1:], lambda i, l: (i, 0, 0))
    qs = pl.BlockSpec((NB, QROWS, 128), lambda i, l: (i, 0, 0))
    return pl.pallas_call(
        functools.partial(attn_body, steps=steps, group=group),
        grid_spec=pltpu.PrefetchScalarGridSpec(num_scalar_prefetch=1, grid=(grid,), in_specs=[qs, new, new, cache, cache], out_specs=[qs, cache, cache]),
        out_shape=[jax.ShapeDtypeStruct((nb, QROWS, 128), BF16), jax.ShapeDtypeStruct(kc.shape, BF16), jax.ShapeDtypeStruct(vc.shape, BF16)],
        compiler_params=pltpu.CompilerParams(vmem_limit_bytes=40 * 1024 * 1024, dimension_semantics=("arbitrary",)),
        cost_estimate=pl.CostEstimate(flops=2 * nb * 32 * 128 * seq * 2, bytes_accessed=4 * nb * half * seq * 2, transcendentals=0),
    )(lengths, q, kn, vn, kc, vc)


def moe_body(h_ref, xm_ref, wr_ref, chb_ref, wact_hbm, wlin_hbm, wdn_hbm, out_ref,
             wcat, wdn, hd, hs, rs1, cs, rs2, lgp, lr1, lcs, lr2, u, ud, pd, yr,
             wsem, s1s, s1r, s2s, s2r, ls, lr, us, ur, ys, yrs, gs, gr):
    experts = wcat.shape[0]
    ff = wact_hbm.shape[2]
    steps = hs.shape[0]
    nb = hs.shape[1]
    hb, qb = nb // 2, nb // 4
    top = chb_ref.shape[0]
    dp, y, x = lax.axis_index("dp"), lax.axis_index("y"), lax.axis_index("x")
    core, chip = x % 2, x // 2
    sib = (dp, y, chip * 2 + (1 - core))
    peer = (dp, y, (1 - chip) * 2 + core)
    ypeer = [None] + [(dp, (y + d) % 4, x) for d in (1, 2, 3)]

    def rcopy(src, dst, ssem, rsem, dev):
        return pltpu.make_async_remote_copy(src_ref=src, dst_ref=dst, send_sem=ssem, recv_sem=rsem, device_id=dev, device_id_type=MESH)

    w0 = pltpu.make_async_copy(wact_hbm, wcat.at[:, :, pl.ds(0, ff)], wsem.at[0])
    w1 = pltpu.make_async_copy(wlin_hbm, wcat.at[:, :, pl.ds(ff, ff)], wsem.at[1])
    w2 = pltpu.make_async_copy(wdn_hbm, wdn, wsem.at[2])
    w0.start()
    w1.start()
    w2.start()

    barrier = pltpu.get_barrier_semaphore()
    for dev in [sib, peer] + ypeer[1:]:
        pl.semaphore_signal(barrier, inc=1, device_id=dev, device_id_type=MESH)
    lg = jnp.dot(h_ref[...], wr_ref[...], preferred_element_type=F32)
    for c in range(steps):
        lgp[c] = lg[c * nb:(c + 1) * nb]
    pl.semaphore_wait(barrier, 5)

    keep = pl.multiple_of(core * hb, hb)
    give = pl.multiple_of((1 - core) * hb, hb)
    sub_keep = pl.multiple_of(chip * qb, qb)
    sub_give = pl.multiple_of((1 - chip) * qb, qb)
    own = pl.multiple_of(core * hb + chip * qb, qb)
    other = pl.multiple_of(core * hb + (1 - chip) * qb, qb)
    sib_own = pl.multiple_of((1 - core) * hb + chip * qb, qb)
    sib_other = pl.multiple_of((1 - core) * hb + (1 - chip) * qb, qb)

    l1 = rcopy(lgp.at[:, pl.ds(give, hb), :], lr1, ls.at[0], lr.at[0], sib)
    l1.start()

    def part_a(c):
        def one(e, carry):
            hd[e] = jnp.dot(h_ref[c * nb:(c + 1) * nb, :], wcat[e], preferred_element_type=F32).astype(BF16)
            return carry
        lax.fori_loop(0, experts, one, 0)

        def pick(i, carry):
            r = pl.multiple_of(i * 16, 16)
            ch = [chb_ref[j, pl.ds(pl.multiple_of(c * nb + i * 16, 16), 16), :] for j in range(top)]
            acc_a = [jnp.zeros((16, ff), BF16) for _ in range(top)]
            acc_l = [jnp.zeros((16, ff), BF16) for _ in range(top)]
            for e in range(experts):
                va = hd[e, pl.ds(r, 16), 0:ff]
                vl = hd[e, pl.ds(r, 16), ff:2 * ff]
                for j in range(top):
                    m = ch[j] == jnp.asarray(e, BF16)
                    acc_a[j] = jnp.where(m, va, acc_a[j])
                    acc_l[j] = jnp.where(m, vl, acc_l[j])
            for j in range(top):
                hs[c, pl.ds(r, 16), 2 * j * ff:(2 * j + 1) * ff] = acc_a[j]
                hs[c, pl.ds(r, 16), (2 * j + 1) * ff:(2 * j + 2) * ff] = acc_l[j]
            return carry
        lax.fori_loop(0, nb // 16, pick, 0)

    def s1(c):
        return rcopy(hs.at[c, pl.ds(give, hb), :], rs1.at[c], s1s.at[c], s1r.at[c], sib)

    def s2(c):
        return rcopy(cs.at[c], rs2.at[c], s2s.at[c], s2r.at[c], peer)

    def part_b(c):
        s1(c).wait_recv()

        def add(i, carry):
            r = pl.multiple_of(i * 16, 16)
            mine = hs[c, pl.ds(pl.multiple_of(keep + sub_give + r, 16), 16), :].astype(F32)
            got = rs1[c, pl.ds(pl.multiple_of(sub_give + r, 16), 16), :].astype(F32)
            cs[c, pl.ds(r, 16), :] = (mine + got).astype(BF16)
            return carry
        lax.fori_loop(0, qb // 16, add, 0)
        s2(c).start()

    def u_peer(c, row):
        return rcopy(u.at[c, pl.ds(row, qb), :], u.at[c, pl.ds(row, qb), :], us.at[c, 0], ur.at[c, 0], peer)

    def u_sib(c, row, k):
        return rcopy(u.at[c, pl.ds(row, qb), :], u.at[c, pl.ds(row, qb), :], us.at[c, k], ur.at[c, k], sib)

    def part_u(c):
        s2(c).wait_recv()

        def tile(i, carry):
            r = pl.multiple_of(i * 16, 16)
            r_own = pl.multiple_of(own + r, 16)
            r_sub = pl.multiple_of(sub_keep + r, 16)
            logit = lgp[c, pl.ds(r_own, 16), :] + lr1[c, pl.ds(r_sub, 16), :] + lr2[c, pl.ds(r, 16), :]
            lane = lax.broadcasted_iota(jnp.int32, (16, 128), 1).astype(F32)
            hit = [chb_ref[j, pl.ds(pl.multiple_of(c * nb + own + r, 16), 16), :].astype(F32) == lane for j in range(top)]
            any_hit = hit[0]
            for j in range(1, top):
                any_hit = any_hit | hit[j]
            peak = jnp.max(jnp.where(any_hit, logit, -jnp.inf), axis=1, keepdims=True)
            ex = jnp.where(any_hit, jnp.exp(logit - peak), 0.0)
            coef = ex / jnp.sum(ex, axis=1, keepdims=True)
            for j in range(top):
                gate = jnp.sum(jnp.where(hit[j], coef, 0.0), axis=1, keepdims=True)
                ca, cl = pl.ds(2 * j * ff, ff), pl.ds((2 * j + 1) * ff, ff)
                act = hs[c, pl.ds(r_own, 16), ca].astype(F32) + rs1[c, pl.ds(r_sub, 16), ca].astype(F32) + rs2[c, pl.ds(r, 16), ca].astype(F32)
                lin = hs[c, pl.ds(r_own, 16), cl].astype(F32) + rs1[c, pl.ds(r_sub, 16), cl].astype(F32) + rs2[c, pl.ds(r, 16), cl].astype(F32)
                val = gate * (act / (1.0 + jnp.exp(-act))) * lin
                u[c, pl.ds(r_own, 16), j * ff:(j + 1) * ff] = val.astype(BF16)
            return carry
        lax.fori_loop(0, qb // 16, tile, 0)
        u_peer(c, own).start()
        u_sib(c, own, 1).start()

    def part_f(c):
        u_peer(c, other).wait_recv()
        u_sib(c, other, 2).start()

    def y_rs(c, d):
        row = pl.multiple_of(((y + d) % 4) * qb, qb)
        return rcopy(pd.at[c, pl.ds(row, qb), :], yr.at[c, 3 - d], ys.at[c, d - 1], yrs.at[c, 3 - d], ypeer[d])

    def y_rs_recv(c, k):
        return rcopy(pd.at[c, pl.ds(0, qb), :], yr.at[c, k], ys.at[c, k], yrs.at[c, k], ypeer[1])

    def part_d(c):
        u_sib(c, sib_own, 1).wait_recv()
        u_sib(c, sib_other, 2).wait_recv()

        def spread(i, carry):
            r = pl.multiple_of(i * 16, 16)
            ch = [chb_ref[j, pl.ds(pl.multiple_of(c * nb + i * 16, 16), 16), :] for j in range(top)]
            vals = [u[c, pl.ds(r, 16), j * ff:(j + 1) * ff] for j in range(top)]
            for e in range(experts):
                acc = jnp.zeros((16, ff), BF16)
                for j in range(top):
                    acc = jnp.where(ch[j] == jnp.asarray(e, BF16), vals[j], acc)
                ud[pl.ds(r, 16), e * ff:(e + 1) * ff] = acc
            return carry
        lax.fori_loop(0, nb // 16, spread, 0)
        pd[c] = jnp.dot(ud[...], wdn[...], preferred_element_type=F32).astype(BF16)
        for d in (1, 2, 3):
            y_rs(c, d).start()

    def y_ag(c, d):
        row = pl.multiple_of(y * qb, qb)
        return rcopy(out_ref.at[c, pl.ds(row, qb), :], out_ref.at[c, pl.ds(row, qb), :], gs.at[c, d - 1], gr.at[c, 3 - d], ypeer[d])

    def y_ag_recv(c, k):
        row = pl.multiple_of(((y + k + 1) % 4) * qb, qb)
        return rcopy(out_ref.at[c, pl.ds(row, qb), :], out_ref.at[c, pl.ds(row, qb), :], gs.at[c, k], gr.at[c, k], ypeer[1])

    def part_g(c):
        for k in range(3):
            y_rs_recv(c, k).wait_recv()
        row = pl.multiple_of(y * qb, qb)
        tot = xm_ref[pl.ds(pl.multiple_of(c * nb + y * qb, qb), qb), :].astype(F32)
        acc = pd[c, pl.ds(row, qb), :].astype(F32)
        for k in range(3):
            acc = acc + yr[c, k].astype(F32)
        out_ref[c, pl.ds(row, qb), :] = (tot + acc).astype(BF16)
        for d in (1, 2, 3):
            y_ag(c, d).start()

    w0.wait()
    w1.wait()
    part_a(0)
    s1(0).start()
    l1.wait_recv()
    lcs[...] = lgp[:, pl.ds(pl.multiple_of(keep + sub_give, qb), qb), :] + lr1[:, pl.ds(sub_give, qb), :]
    l2 = rcopy(lcs, lr2, ls.at[1], lr.at[1], peer)
    l2.start()
    part_b(0)
    part_a(1)
    s1(1).start()
    l2.wait_recv()
    part_u(0)
    part_b(1)
    part_a(2)
    s1(2).start()
    part_f(0)
    part_u(1)
    part_b(2)
    w2.wait()
    part_d(0)
    part_f(1)
    part_d(1)
    part_u(2)
    part_g(0)
    part_g(1)
    part_f(2)
    part_d(2)
    part_g(2)
    for c in range(steps):
        for k in range(3):
            y_ag_recv(c, k).wait_recv()
    l1.wait_send()
    l2.wait_send()
    for c in range(steps):
        s1(c).wait_send()
        s2(c).wait_send()
        u_peer(c, own).wait_send()
        u_sib(c, own, 1).wait_send()
        u_sib(c, other, 2).wait_send()
        for d in (1, 2, 3):
            y_rs(c, d).wait_send()
            y_ag(c, d).wait_send()


def moe(h2, x_mid, w_router, chb, w_act, w_lin, w_down, steps):
    rows, width = h2.shape
    nb = rows // steps
    experts, _, ff = w_act.shape
    top = chb.shape[0]
    hb, qb = nb // 2, nb // 4
    dma = pltpu.SemaphoreType.DMA
    vm = pl.BlockSpec(memory_space=pltpu.VMEM)
    hbm = pl.BlockSpec(memory_space=pl.ANY)
    return pl.pallas_call(
        moe_body,
        out_shape=jax.ShapeDtypeStruct((steps, nb, width), BF16),
        in_specs=[vm, vm, vm, vm, hbm, hbm, hbm],
        out_specs=vm,
        scratch_shapes=[
            pltpu.VMEM((experts, width, 2 * ff), BF16),
            pltpu.VMEM((experts * ff, width), BF16),
            pltpu.VMEM((experts, nb, 2 * ff), BF16),
            pltpu.VMEM((steps, nb, 2 * top * ff), BF16),
            pltpu.VMEM((steps, hb, 2 * top * ff), BF16),
            pltpu.VMEM((steps, qb, 2 * top * ff), BF16),
            pltpu.VMEM((steps, qb, 2 * top * ff), BF16),
            pltpu.VMEM((steps, nb, 128), F32),
            pltpu.VMEM((steps, hb, 128), F32),
            pltpu.VMEM((steps, qb, 128), F32),
            pltpu.VMEM((steps, qb, 128), F32),
            pltpu.VMEM((steps, nb, top * ff), BF16),
            pltpu.VMEM((nb, experts * ff), BF16),
            pltpu.VMEM((steps, nb, width), BF16),
            pltpu.VMEM((steps, 3, qb, width), BF16),
            dma((3,)), dma((steps,)), dma((steps,)), dma((steps,)), dma((steps,)),
            dma((2,)), dma((2,)), dma((steps, 3)), dma((steps, 3)),
            dma((steps, 3)), dma((steps, 3)), dma((steps, 3)), dma((steps, 3)),
        ],
        compiler_params=pltpu.CompilerParams(collective_id=1, has_side_effects=True, vmem_limit_bytes=56 * 1024 * 1024),
        cost_estimate=pl.CostEstimate(flops=6 * rows * width * experts * ff, bytes_accessed=12 * 1024 * 1024, transcendentals=0),
    )(h2, x_mid, w_router, chb, w_act, w_lin, w_down.reshape(experts * ff, width))


def shard_norm(x_val, gain_vec, width_full):
    x_f32 = x_val.astype(F32)
    sq_total = lax.psum(jnp.sum(x_f32 * x_f32, axis=-1, keepdims=True), 'x')
    return (x_f32 * lax.rsqrt(sq_total / width_full + EPS) * gain_vec.astype(F32)).astype(BF16)


def rotate(vectors, positions):
    head_dim = vectors.shape[-1]
    half_dim = head_dim // 2
    inv_freq = ROPE_BASE ** (-(jnp.arange(half_dim, dtype=F32) * 2.0 / head_dim))
    angle_shape = (vectors.shape[0],) + (1,) * (vectors.ndim - 2) + (half_dim,)
    angles = (positions.astype(F32)[:, None] * inv_freq[None, :]).reshape(angle_shape)
    cosine = jnp.cos(angles)
    sine_val = jnp.sin(angles)
    first_half = vectors[..., :half_dim].astype(F32)
    second_half = vectors[..., half_dim:].astype(F32)
    return jnp.concatenate([first_half * cosine - second_half * sine_val, second_half * cosine + first_half * sine_val], axis=-1).astype(BF16)


def solution(mesh):
    x_count = mesh.shape['x']
    cache_spec = P('dp', None, 'y', None)
    in_specs = (P(None, 'dp'), P('dp'), P(None, 'dp', None), P(None, 'x'), cache_spec, cache_spec, P('x'), P('x', 'y'), P('x', 'y'), P('x', 'y'), P('y', 'x'), P('x'), P('x', None), P(None, 'x', 'y'), P(None, 'x', 'y'), P(None, 'y', 'x'))
    out_specs = (P(None, 'dp', 'x'), cache_spec, cache_spec)

    def per_device(tokens, lengths, choices, emb_table, k_cache, v_cache, g_attn, w_q, w_k, w_v, w_o, g_ffn, w_router, w_act, w_lin, w_down):
        steps, nb = tokens.shape
        seq, kvl, hdim = k_cache.shape[1:]
        q_cols, kv_cols = w_q.shape[1], w_k.shape[1]
        width = emb_table.shape[1]
        width_full = width * x_count
        group = q_cols // kv_cols
        rows = steps * nb
        top = choices.shape[2]
        positions = (lengths[None, :] + jnp.arange(steps, dtype=lengths.dtype)[:, None]).reshape(rows)
        wq = w_q.reshape(width, kvl, group, hdim).transpose(0, 2, 1, 3).reshape(width, q_cols)
        wo = w_o.reshape(kvl, group, hdim, width).transpose(1, 0, 2, 3).reshape(q_cols, width)
        w_all = jnp.concatenate([wq, w_k, w_v], axis=1)
        chb = jnp.broadcast_to(choices.reshape(rows, top).T.astype(BF16)[:, :, None], (top, rows, 128))
        wr = jnp.pad(w_router, ((0, 0), (0, 128 - w_router.shape[1])))

        x_in = jnp.take(emb_table, tokens.reshape(rows), axis=0)
        normed = shard_norm(x_in, g_attn, width_full)
        proj = lax.psum(jnp.dot(normed, w_all, preferred_element_type=F32).astype(BF16), 'x')
        heads = q_cols // hdim
        qk = rotate(proj[:, :q_cols + kv_cols].reshape(rows, heads + kvl, hdim), positions)
        q = qk[:, :heads].reshape(steps, nb, group, kvl * hdim).transpose(1, 0, 2, 3).reshape(nb, steps * group, kvl * hdim)
        q = jnp.pad(q, ((0, 0), (0, QROWS - steps * group), (0, 0)))
        kn = qk[:, heads:].reshape(steps, nb, kv_cols).transpose(1, 0, 2).reshape(nb // NB, NB * steps, kv_cols)
        vn = proj[:, q_cols + kv_cols:].reshape(steps, nb, kv_cols).transpose(1, 0, 2).reshape(nb // NB, NB * steps, kv_cols)
        pad = 32 - NB * steps
        kn = jnp.pad(kn, ((0, 0), (0, pad), (0, 0)))
        vn = jnp.pad(vn, ((0, 0), (0, pad), (0, 0)))
        kc = k_cache.transpose(0, 2, 3, 1).reshape(nb, kv_cols, seq)
        vc = v_cache.transpose(0, 2, 3, 1).reshape(nb, kv_cols, seq)
        o, ko, vo = attention(lengths, q, kn, vn, kc, vc, steps, group)
        mixed = o[:, :steps * group].reshape(nb, steps, q_cols).transpose(1, 0, 2).reshape(rows, q_cols)
        attn = lax.psum(jnp.dot(mixed, wo, preferred_element_type=F32).astype(BF16), 'y')
        x_mid = (x_in.astype(F32) + attn.astype(F32)).astype(BF16)
        h2 = shard_norm(x_mid, g_ffn, width_full)
        hidden = moe(h2, x_mid, wr, chb, w_act, w_lin, w_down, steps)
        ko = ko.reshape(nb, kvl, hdim, seq).transpose(0, 3, 1, 2)
        vo = vo.reshape(nb, kvl, hdim, seq).transpose(0, 3, 1, 2)
        return hidden, ko, vo

    return jax.shard_map(per_device, mesh=mesh, in_specs=in_specs, out_specs=out_specs, check_vma=False)
```

```python
import functools
import jax
import jax.numpy as jnp
from jax import lax
from jax.experimental import pallas as pl
from jax.experimental.pallas import tpu as pltpu
from jax.sharding import PartitionSpec as P

EPS = 1e-5
ROPE_BASE = 1.0e6
MESH = pl.DeviceIdType.MESH
F32 = jnp.float32
BF16 = jnp.bfloat16
LANE = 128
SUB = 16
MIB = 1024 * 1024
LOWEST = -1.0e30
NB = 16
QROWS = 16


def attn_body(len_ref, q_ref, kn_ref, vn_ref, k_ref, v_ref, o_ref, ko_ref, vo_ref, s_ref, w_ref, *, steps, group):
    half, seq = k_ref.shape[1:]
    n_seq = k_ref.shape[0]
    step = pl.program_id(0)
    fill = jnp.zeros((LANE - kn_ref.shape[1], LANE), F32)
    kn_t = jnp.concatenate([kn_ref[0].astype(F32), fill], axis=0).T
    vn_t = jnp.concatenate([vn_ref[0].astype(F32), fill], axis=0).T
    lane = lax.broadcasted_iota(jnp.int32, (SUB, LANE), 1).astype(F32).astype(BF16)
    srow = lax.broadcasted_iota(jnp.int32, (2 * QROWS, seq), 0)
    scol = lax.broadcasted_iota(jnp.int32, (2 * QROWS, seq), 1)
    srow = jnp.where(srow >= QROWS, srow - QROWS, srow)
    rel = scol - jnp.where(srow >= 2 * group, 2, jnp.where(srow >= group, 1, 0))
    low = lax.broadcasted_iota(jnp.int32, (QROWS, LANE), 1) < 64
    low_b = lane < jnp.asarray(64, BF16)
    for b in range(n_seq):
        pos = len_ref[step * n_seq + b]
        turn = lax.rem(pos + LANE - b * steps, LANE)
        new = (pltpu.roll(kn_t, turn, 1).astype(BF16), pltpu.roll(vn_t, turn, 1).astype(BF16))
        gap = lane - jnp.full((SUB, LANE), pos.astype(F32), F32).astype(BF16)
        for tile in range(seq // LANE):
            lo = jnp.asarray(-LANE * tile, BF16)
            hi = jnp.asarray(steps - 1 - LANE * tile, BF16)
            hit = (gap >= lo) & (gap <= hi)
            for i in range(half // SUB):
                rs, cs = slice(SUB * i, SUB * i + SUB), slice(LANE * tile, LANE * tile + LANE)
                ko_ref[b, rs, cs] = jnp.where(hit, new[0][rs], k_ref[b, rs, cs])
                vo_ref[b, rs, cs] = jnp.where(hit, new[1][rs], v_ref[b, rs, cs])
    for b in range(n_seq):
        q16 = q_ref[b]
        zero = jnp.zeros_like(q16)
        q32 = jnp.concatenate([jnp.where(low_b, q16, zero), jnp.where(low_b, zero, q16)], axis=0)
        s_ref[b] = jnp.dot(q32, ko_ref[b], preferred_element_type=F32)
    tots = []
    for b in range(n_seq):
        pos = len_ref[step * n_seq + b]
        ok = rel <= pos
        s = jnp.where(ok, s_ref[b] * 0.125, LOWEST)
        peak = jnp.max(s, axis=1, keepdims=True)
        w = jnp.where(ok, jnp.exp(s - peak), 0.0)
        tots.append(jnp.sum(w, axis=1, keepdims=True))
        w_ref[b] = w.astype(BF16)
    for b in range(n_seq):
        o = lax.dot_general(w_ref[b], vo_ref[b], (((1,), (1,)), ((), ())), preferred_element_type=F32)
        o = o / tots[b]
        o_ref[b] = jnp.where(low, o[:QROWS], o[QROWS:]).astype(BF16)


def attention(lengths, q, kn, vn, kc, vc, steps, group):
    nb, half, seq = kc.shape
    grid = nb // NB
    cache = pl.BlockSpec((NB, half, seq), lambda i, l: (i, 0, 0))
    new = pl.BlockSpec((1,) + kn.shape[1:], lambda i, l: (i, 0, 0))
    qs = pl.BlockSpec((NB, QROWS, LANE), lambda i, l: (i, 0, 0))
    return pl.pallas_call(
        functools.partial(attn_body, steps=steps, group=group),
        grid_spec=pltpu.PrefetchScalarGridSpec(num_scalar_prefetch=1, grid=(grid,), in_specs=[qs, new, new, cache, cache], out_specs=[qs, cache, cache], scratch_shapes=[pltpu.VMEM((NB, 2 * QROWS, seq), F32), pltpu.VMEM((NB, 2 * QROWS, seq), BF16)]),
        out_shape=[jax.ShapeDtypeStruct((nb, QROWS, LANE), BF16), jax.ShapeDtypeStruct(kc.shape, BF16), jax.ShapeDtypeStruct(vc.shape, BF16)],
        compiler_params=pltpu.CompilerParams(vmem_limit_bytes=40 * MIB, dimension_semantics=("arbitrary",)),
        cost_estimate=pl.CostEstimate(flops=2 * nb * 32 * LANE * seq * 2, bytes_accessed=4 * nb * half * seq * 2, transcendentals=0),
    )(lengths, q, kn, vn, kc, vc)


def remote(src, dst, ssem, rsem, dev):
    return pltpu.make_async_remote_copy(src_ref=src, dst_ref=dst, send_sem=ssem, recv_sem=rsem, device_id=dev, device_id_type=MESH)


def square_rows(x_f32):
    tiles = x_f32.shape[1] // LANE
    acc = x_f32[:, 0:LANE] * x_f32[:, 0:LANE]
    for i in range(1, tiles):
        part = x_f32[:, LANE * i:LANE * (i + 1)]
        acc = acc + part * part
    return jnp.sum(acc.T, axis=0, keepdims=True)


def scale_rows(x_f32, stat_row, gain, width_full):
    scale = lax.rsqrt(stat_row / width_full + EPS)
    col = jnp.broadcast_to(scale, (LANE, LANE)).T
    parts = [x_f32[:, LANE * i:LANE * (i + 1)] * col * gain[:, LANE * i:LANE * (i + 1)] for i in range(x_f32.shape[1] // LANE)]
    return jnp.concatenate(parts, axis=1).astype(BF16)


def front_body(x_ref, g_ref, w_ref, cos_ref, sin_ref, out_ref, st, st_in, hh, pj, rs1, cs, rs2, sts, str_, s1s, s1r, s2s, s2r, s3s, s3r, *, width_full, turn_cols):
    steps, nb = out_ref.shape[:2]
    cols = out_ref.shape[2]
    hb = nb // 2
    dp, y, x = lax.axis_index("dp"), lax.axis_index("y"), lax.axis_index("x")
    core, chip = x % 2, x // 2
    sib = (dp, y, chip * 2 + (1 - core))
    peer = (dp, y, (1 - chip) * 2 + core)
    diag = (dp, y, (1 - chip) * 2 + (1 - core))
    near = (sib, peer, diag)
    barrier = pltpu.get_barrier_semaphore()
    for dev in near:
        pl.semaphore_signal(barrier, inc=1, device_id=dev, device_id_type=MESH)
    keep = pl.multiple_of(core * hb, hb)
    give = pl.multiple_of((1 - core) * hb, hb)
    st[...] = jnp.zeros_like(st)
    blocks = steps * nb // LANE
    for i in range(blocks):
        st[i:i + 1, :] = square_rows(x_ref[LANE * i:LANE * (i + 1), :].astype(F32))
    pl.semaphore_wait(barrier, 3)
    stat = [remote(st, st_in.at[k], sts.at[k], str_.at[k], near[k]) for k in range(3)]
    for k in range(3):
        stat[k].start()
    for k in range(3):
        stat[k].wait_recv()
    total = st[...] + st_in[0] + st_in[1] + st_in[2]

    def s1(c):
        return remote(pj.at[c, pl.ds(give, hb), :], rs1.at[c], s1s.at[c], s1r.at[c], sib)

    def s2(c):
        return remote(cs.at[c], rs2.at[c], s2s.at[c], s2r.at[c], peer)

    def s3(c, row):
        return remote(out_ref.at[c, pl.ds(row, hb), :], out_ref.at[c, pl.ds(row, hb), :], s3s.at[c], s3r.at[c], sib)

    def mid(c):
        s1(c).wait_recv()
        cs[c] = (pj[c, pl.ds(keep, hb), :].astype(F32) + rs1[c].astype(F32)).astype(BF16)
        s2(c).start()

    def last(c):
        s2(c).wait_recv()
        fin = (cs[c].astype(F32) + rs2[c].astype(F32)).astype(BF16).astype(F32)
        cosv = cos_ref[c, pl.ds(keep, hb), :]
        sinv = sin_ref[c, pl.ds(keep, hb), :]
        first = lax.broadcasted_iota(jnp.int32, (hb, LANE), 1) % 64 < 32
        for i in range(cols // LANE):
            v = fin[:, LANE * i:LANE * (i + 1)]
            if i < turn_cols // LANE:
                swap = jnp.where(first, pltpu.roll(v, 96, 1), pltpu.roll(v, 32, 1))
                v = v * cosv + swap * sinv
            out_ref[c, pl.ds(keep, hb), LANE * i:LANE * (i + 1)] = v.astype(BF16)
        s3(c, keep).start()

    for c in range(steps):
        for i in range(c * nb // LANE, (c + 1) * nb // LANE):
            hh[LANE * i:LANE * (i + 1), :] = scale_rows(x_ref[LANE * i:LANE * (i + 1), :].astype(F32), total[i:i + 1, :], g_ref[...], width_full)
        pj[c] = jnp.dot(hh[c * nb:(c + 1) * nb, :], w_ref[...], preferred_element_type=F32).astype(BF16)
        s1(c).start()
        if c >= 1:
            mid(c - 1)
    mid(steps - 1)
    for c in range(steps):
        last(c)
    for c in range(steps):
        s3(c, give).wait_recv()
    for k in range(3):
        stat[k].wait_send()
    for c in range(steps):
        s1(c).wait_send()
        s2(c).wait_send()
        s3(c, keep).wait_send()


def front(x_in, gain, w_all, cosv, sinv, steps, width_full, turn_cols):
    rows, width = x_in.shape
    nb = rows // steps
    cols = w_all.shape[1]
    hb = nb // 2
    dma = pltpu.SemaphoreType.DMA
    vm = pl.BlockSpec(memory_space=pltpu.VMEM)
    return pl.pallas_call(
        functools.partial(front_body, width_full=width_full, turn_cols=turn_cols),
        out_shape=jax.ShapeDtypeStruct((steps, nb, cols), BF16),
        in_specs=[vm] * 5,
        out_specs=vm,
        scratch_shapes=[
            pltpu.VMEM((8, LANE), F32), pltpu.VMEM((3, 8, LANE), F32),
            pltpu.VMEM((rows, width), BF16), pltpu.VMEM((steps, nb, cols), BF16),
            pltpu.VMEM((steps, hb, cols), BF16), pltpu.VMEM((steps, hb, cols), BF16), pltpu.VMEM((steps, hb, cols), BF16),
            dma((3,)), dma((3,)), dma((steps,)), dma((steps,)), dma((steps,)), dma((steps,)), dma((steps,)), dma((steps,)),
        ],
        compiler_params=pltpu.CompilerParams(collective_id=2, has_side_effects=True, vmem_limit_bytes=24 * MIB),
        cost_estimate=pl.CostEstimate(flops=2 * rows * width * cols, bytes_accessed=4 * MIB, transcendentals=0),
    )(x_in, gain, w_all, cosv, sinv)


def tail_body(mix_ref, wo_ref, xin_ref, g_ref, wr_ref, chb_ref, wact_hbm, wlin_hbm, wdn_hbm, out_ref,
              wcat, wdn, pa, ar, xm, hh, st, st_in, hs, rs1, cs, rs2, lgp, lr1, lcs, lr2, u, pd, yr,
              wsem, as_, ar_s, xs, xr, sts, str_, s1s, s1r, s2s, s2r, l1s, l1r, l2s, l2r, us, ur, ys, yrs, gs, gr, *, width_full):
    experts = wcat.shape[0]
    ff = wact_hbm.shape[2]
    steps, nb = hs.shape[:2]
    hb, qb = nb // 2, nb // 4
    top = chb_ref.shape[0]
    dp, y, x = lax.axis_index("dp"), lax.axis_index("y"), lax.axis_index("x")
    core, chip = x % 2, x // 2
    sib = (dp, y, chip * 2 + (1 - core))
    peer = (dp, y, (1 - chip) * 2 + core)
    diag = (dp, y, (1 - chip) * 2 + (1 - core))
    near = (sib, peer, diag)
    ypeer = [None] + [(dp, (y + d) % 4, x) for d in (1, 2, 3)]

    w0 = pltpu.make_async_copy(wact_hbm, wcat.at[:, :, pl.ds(0, ff)], wsem.at[0])
    w1 = pltpu.make_async_copy(wlin_hbm, wcat.at[:, :, pl.ds(ff, ff)], wsem.at[1])
    w2 = pltpu.make_async_copy(wdn_hbm, wdn, wsem.at[2])
    barrier = pltpu.get_barrier_semaphore()
    for dev in near + tuple(ypeer[1:]):
        pl.semaphore_signal(barrier, inc=1, device_id=dev, device_id_type=MESH)

    keep = pl.multiple_of(core * hb, hb)
    give = pl.multiple_of((1 - core) * hb, hb)
    sub_keep = pl.multiple_of(chip * qb, qb)
    sub_give = pl.multiple_of((1 - chip) * qb, qb)
    own = pl.multiple_of(core * hb + chip * qb, qb)
    other = pl.multiple_of(core * hb + (1 - chip) * qb, qb)
    sib_own = pl.multiple_of((1 - core) * hb + chip * qb, qb)
    sib_other = pl.multiple_of((1 - core) * hb + (1 - chip) * qb, qb)
    yrow = pl.multiple_of(y * qb, qb)

    def yblock(k):
        return pl.multiple_of(((y + k) % 4) * qb, qb)

    def rs_send(buf, land, ssem, rsem, c, d):
        return remote(buf.at[c, pl.ds(yblock(d), qb), :], land.at[c, 3 - d], ssem.at[c, d - 1], rsem.at[c, 3 - d], ypeer[d])

    def rs_recv(buf, land, ssem, rsem, c, k):
        return remote(buf.at[c, pl.ds(0, qb), :], land.at[c, k], ssem.at[c, k], rsem.at[c, k], ypeer[1])

    def ag_send(buf, ssem, rsem, c, d):
        return remote(buf.at[c, pl.ds(yrow, qb), :], buf.at[c, pl.ds(yrow, qb), :], ssem.at[c, d - 1], rsem.at[c, 3 - d], ypeer[d])

    def ag_recv(buf, ssem, rsem, c, k):
        row = yblock(k + 1)
        return remote(buf.at[c, pl.ds(row, qb), :], buf.at[c, pl.ds(row, qb), :], ssem.at[c, k], rsem.at[c, k], ypeer[1])

    def s1(c):
        return remote(hs.at[c, pl.ds(give, hb), :], rs1.at[c], s1s.at[c], s1r.at[c], sib)

    def s2(c):
        return remote(cs.at[c], rs2.at[c], s2s.at[c], s2r.at[c], peer)

    def l1(c):
        return remote(lgp.at[c, pl.ds(give, hb), :], lr1.at[c], l1s.at[c], l1r.at[c], sib)

    def l2(c):
        return remote(lcs.at[c], lr2.at[c], l2s.at[c], l2r.at[c], peer)

    def u_peer(c, row):
        return remote(u.at[c, pl.ds(row, qb), :], u.at[c, pl.ds(row, qb), :], us.at[c, 0], ur.at[c, 0], peer)

    def u_sib(c, row, k):
        return remote(u.at[c, pl.ds(row, qb), :], u.at[c, pl.ds(row, qb), :], us.at[c, k], ur.at[c, k], sib)

    def stat(c, k):
        return remote(st.at[c], st_in.at[c, k], sts.at[c, k], str_.at[c, k], near[k])

    def attn_out(c):
        pa[c] = jnp.dot(mix_ref[c * nb:(c + 1) * nb, :], wo_ref[...], preferred_element_type=F32).astype(BF16)

    def attn_send(c):
        for d in (1, 2, 3):
            rs_send(pa, ar, as_, ar_s, c, d).start()

    def attn_sum(c):
        for k in range(3):
            rs_recv(pa, ar, as_, ar_s, c, k).wait_recv()
        acc = pa[c, pl.ds(yrow, qb), :].astype(F32)
        for k in range(3):
            acc = acc + ar[c, k].astype(F32)
        base = xin_ref[pl.ds(pl.multiple_of(c * nb + yrow, qb), qb), :].astype(F32)
        xm[c, pl.ds(yrow, qb), :] = (base + acc).astype(BF16)
        for d in (1, 2, 3):
            ag_send(xm, xs, xr, c, d).start()

    def stats(c):
        for k in range(3):
            ag_recv(xm, xs, xr, c, k).wait_recv()
        for i in range(nb // LANE):
            st[c, i:i + 1, :] = square_rows(xm[c, LANE * i:LANE * (i + 1), :].astype(F32))
        for k in range(3):
            stat(c, k).start()

    def norm(c):
        for k in range(3):
            stat(c, k).wait_recv()
        total = st[c] + st_in[c, 0] + st_in[c, 1] + st_in[c, 2]
        for i in range(nb // LANE):
            hh[c, LANE * i:LANE * (i + 1), :] = scale_rows(xm[c, LANE * i:LANE * (i + 1), :].astype(F32), total[i:i + 1, :], g_ref[...], width_full)
        lgp[c] = jnp.dot(hh[c], wr_ref[...], preferred_element_type=F32)
        l1(c).start()

    def experts_in(c, hd):
        span = 4

        def few(i, carry):
            for k in range(span):
                e = i * span + k
                hval = jnp.dot(hh[c], wcat[e], preferred_element_type=F32)
                hd[e, :, 0:ff] = hval[:, 0:ff].astype(BF16)
                hd[experts + e, :, 0:ff] = hval[:, ff:2 * ff].astype(BF16)
            return carry
        lax.fori_loop(0, experts // span, few, 0)

    def pick(c, hd, chs):
        def tile(i, carry):
            r = pl.multiple_of(i * SUB, SUB)
            ch = [chs[j, pl.ds(pl.multiple_of(c * nb + i * SUB, SUB), SUB), :] for j in range(top)]
            span = 8

            def some(g, state):
                acc, ev = list(state[0]), state[1]
                for k in range(span):
                    e = g * span + k
                    va = hd[e, pl.ds(r, SUB), :]
                    vl = hd[experts + e, pl.ds(r, SUB), :]
                    for j in range(top):
                        m = ch[j] == ev
                        acc[2 * j] = jnp.where(m, va, acc[2 * j])
                        acc[2 * j + 1] = jnp.where(m, vl, acc[2 * j + 1])
                    ev = ev + jnp.ones_like(ev)
                return tuple(acc), ev
            zero = jnp.zeros((SUB, ff), BF16)
            acc, _ = lax.fori_loop(0, experts // span, some, (tuple(zero for _ in range(2 * top)), zero))
            for k in range(2 * top):
                hs[c, pl.ds(r, SUB), k * ff:(k + 1) * ff] = acc[k]
            return carry
        lax.fori_loop(0, nb // SUB, tile, 0)

    def logits_mid(c):
        l1(c).wait_recv()
        lcs[c] = lgp[c, pl.ds(other, qb), :] + lr1[c, pl.ds(sub_give, qb), :]
        l2(c).start()

    def part_b(c):
        s1(c).wait_recv()

        def add(i, carry):
            r = pl.multiple_of(i * SUB, SUB)
            mine = hs[c, pl.ds(pl.multiple_of(other + r, SUB), SUB), :].astype(F32)
            got = rs1[c, pl.ds(pl.multiple_of(sub_give + r, SUB), SUB), :].astype(F32)
            cs[c, pl.ds(r, SUB), :] = (mine + got).astype(BF16)
            return carry
        lax.fori_loop(0, qb // SUB, add, 0)
        s2(c).start()

    def part_u(c):
        l2(c).wait_recv()
        s2(c).wait_recv()

        def tile(i, carry):
            r = pl.multiple_of(i * SUB, SUB)
            r_own = pl.multiple_of(own + r, SUB)
            r_sub = pl.multiple_of(sub_keep + r, SUB)
            logit = lgp[c, pl.ds(r_own, SUB), :] + lr1[c, pl.ds(r_sub, SUB), :] + lr2[c, pl.ds(r, SUB), :]
            lane = lax.broadcasted_iota(jnp.int32, (SUB, LANE), 1).astype(F32)
            hit = [chb_ref[j, pl.ds(pl.multiple_of(c * nb + own + r, SUB), SUB), :].astype(F32) == lane for j in range(top)]
            any_hit = hit[0]
            for j in range(1, top):
                any_hit = any_hit | hit[j]
            peak = jnp.max(jnp.where(any_hit, logit, -jnp.inf), axis=1, keepdims=True)
            ex = jnp.where(any_hit, jnp.exp(logit - peak), 0.0)
            coef = ex / jnp.sum(ex, axis=1, keepdims=True)
            for j in range(top):
                gate = jnp.sum(jnp.where(hit[j], coef, 0.0), axis=1, keepdims=True)
                ca, cl = pl.ds(2 * j * ff, ff), pl.ds((2 * j + 1) * ff, ff)
                act = hs[c, pl.ds(r_own, SUB), ca].astype(F32) + rs1[c, pl.ds(r_sub, SUB), ca].astype(F32) + rs2[c, pl.ds(r, SUB), ca].astype(F32)
                lin = hs[c, pl.ds(r_own, SUB), cl].astype(F32) + rs1[c, pl.ds(r_sub, SUB), cl].astype(F32) + rs2[c, pl.ds(r, SUB), cl].astype(F32)
                val = gate * (act / (1.0 + jnp.exp(-act))) * lin
                u[c, pl.ds(r_own, SUB), j * ff:(j + 1) * ff] = val.astype(BF16)
            return carry
        lax.fori_loop(0, qb // SUB, tile, 0)
        u_peer(c, own).start()
        u_sib(c, own, 1).start()

    def part_f(c):
        u_peer(c, other).wait_recv()
        u_sib(c, other, 2).start()

    def part_d(c, ud, chs, us16):
        u_sib(c, sib_own, 1).wait_recv()
        u_sib(c, sib_other, 2).wait_recv()
        for j in range(top):
            us16[j] = u[c, :, j * ff:(j + 1) * ff]

        def spread(i, carry):
            r = pl.multiple_of(i * SUB, SUB)
            ch = [chs[j, pl.ds(pl.multiple_of(c * nb + i * SUB, SUB), SUB), :] for j in range(top)]
            vals = [us16[j, pl.ds(r, SUB), :] for j in range(top)]
            for e in range(experts):
                acc = jnp.zeros((SUB, ff), BF16)
                for j in range(top):
                    acc = jnp.where(ch[j] == jnp.asarray(e, BF16), vals[j], acc)
                ud[pl.ds(r, SUB), e * ff:(e + 1) * ff] = acc
            return carry
        lax.fori_loop(0, nb // SUB, spread, 0)
        pd[c] = jnp.dot(ud[...], wdn[...], preferred_element_type=F32).astype(BF16)
        for d in (1, 2, 3):
            rs_send(pd, yr, ys, yrs, c, d).start()

    def part_g(c):
        for k in range(3):
            rs_recv(pd, yr, ys, yrs, c, k).wait_recv()
        acc = pd[c, pl.ds(yrow, qb), :].astype(F32)
        for k in range(3):
            acc = acc + yr[c, k].astype(F32)
        out_ref[c, pl.ds(yrow, qb), :] = (xm[c, pl.ds(yrow, qb), :].astype(F32) + acc).astype(BF16)
        for d in (1, 2, 3):
            ag_send(out_ref, gs, gr, c, d).start()

    def run(hd, ud, chs, us16):
        attn_out(0)
        pl.semaphore_wait(barrier, 6)
        attn_send(0)
        attn_out(1)
        attn_send(1)
        w0.start()
        w1.start()
        w2.start()
        st[...] = jnp.zeros_like(st)
        for j in range(top):
            chs[j] = chb_ref[j]
        attn_out(2)
        attn_sum(0)
        attn_send(2)
        attn_sum(1)
        attn_sum(2)
        stats(0)
        norm(0)
        w0.wait()
        w1.wait()
        experts_in(0, hd)
        logits_mid(0)
        stats(1)
        pick(0, hd, chs)
        s1(0).start()
        norm(1)
        stats(2)
        experts_in(1, hd)
        part_b(0)
        logits_mid(1)
        norm(2)
        pick(1, hd, chs)
        s1(1).start()
        experts_in(2, hd)
        part_u(0)
        part_b(1)
        logits_mid(2)
        pick(2, hd, chs)
        s1(2).start()
        part_f(0)
        part_u(1)
        part_b(2)
        w2.wait()
        part_d(0, ud, chs, us16)
        part_f(1)
        part_u(2)
        part_d(1, ud, chs, us16)
        part_f(2)
        part_g(0)
        part_d(2, ud, chs, us16)
        part_g(1)
        part_g(2)

    bf = functools.partial(pltpu.VMEM, dtype=BF16)
    pl.run_scoped(run, bf((2 * experts, nb, ff)), bf((nb, experts * ff)), bf((top, steps * nb, ff)), bf((top, nb, ff)))

    for c in range(steps):
        for k in range(3):
            ag_recv(out_ref, gs, gr, c, k).wait_recv()
    for c in range(steps):
        l1(c).wait_send()
        l2(c).wait_send()
        s1(c).wait_send()
        s2(c).wait_send()
        u_peer(c, own).wait_send()
        u_sib(c, own, 1).wait_send()
        u_sib(c, other, 2).wait_send()
        for k in range(3):
            stat(c, k).wait_send()
        for d in (1, 2, 3):
            rs_send(pa, ar, as_, ar_s, c, d).wait_send()
            ag_send(xm, xs, xr, c, d).wait_send()
            rs_send(pd, yr, ys, yrs, c, d).wait_send()
            ag_send(out_ref, gs, gr, c, d).wait_send()


def tail(mixed, wo, x_in, gain, w_router, chb, w_act, w_lin, w_down, steps, width_full):
    rows, width = x_in.shape
    nb = rows // steps
    experts, _, ff = w_act.shape
    top = chb.shape[0]
    hb, qb = nb // 2, nb // 4
    dma = pltpu.SemaphoreType.DMA
    vm = pl.BlockSpec(memory_space=pltpu.VMEM)
    hbm = pl.BlockSpec(memory_space=pl.ANY)
    sems = [(steps, 3)] * 6 + [(steps,)] * 8 + [(steps, 3)] * 6
    return pl.pallas_call(
        functools.partial(tail_body, width_full=width_full),
        out_shape=jax.ShapeDtypeStruct((steps, nb, width), BF16),
        in_specs=[vm] * 6 + [hbm] * 3,
        out_specs=vm,
        scratch_shapes=[
            pltpu.VMEM((experts, width, 2 * ff), BF16),
            pltpu.VMEM((experts * ff, width), BF16),
            pltpu.VMEM((steps, nb, width), BF16),
            pltpu.VMEM((steps, 3, qb, width), BF16),
            pltpu.VMEM((steps, nb, width), BF16),
            pltpu.VMEM((steps, nb, width), BF16),
            pltpu.VMEM((steps, 8, LANE), F32),
            pltpu.VMEM((steps, 3, 8, LANE), F32),
            pltpu.VMEM((steps, nb, 2 * top * ff), BF16),
            pltpu.VMEM((steps, hb, 2 * top * ff), BF16),
            pltpu.VMEM((steps, qb, 2 * top * ff), BF16),
            pltpu.VMEM((steps, qb, 2 * top * ff), BF16),
            pltpu.VMEM((steps, nb, LANE), F32),
            pltpu.VMEM((steps, hb, LANE), F32),
            pltpu.VMEM((steps, qb, LANE), F32),
            pltpu.VMEM((steps, qb, LANE), F32),
            pltpu.VMEM((steps, nb, top * ff), BF16),
            pltpu.VMEM((steps, nb, width), BF16),
            pltpu.VMEM((steps, 3, qb, width), BF16),
            dma((3,)),
        ] + [dma(n) for n in sems],
        compiler_params=pltpu.CompilerParams(collective_id=1, has_side_effects=True, vmem_limit_bytes=60 * MIB),
        cost_estimate=pl.CostEstimate(flops=6 * rows * width * experts * ff, bytes_accessed=12 * MIB, transcendentals=0),
    )(mixed, wo, x_in, gain, w_router, chb, w_act, w_lin, w_down.reshape(experts * ff, width))


def turn_tables(positions, head_dim):
    half_dim = head_dim // 2
    inv_freq = ROPE_BASE ** (-(jnp.arange(half_dim, dtype=F32) * 2.0 / head_dim))
    angles = positions.astype(F32)[:, None] * inv_freq[None, :]
    cosine, sine_val = jnp.cos(angles), jnp.sin(angles)
    return jnp.tile(cosine, (1, 4)), jnp.tile(jnp.concatenate([-sine_val, sine_val], axis=1), (1, 2))


def solution(mesh):
    x_count = mesh.shape['x']
    cache_spec = P('dp', None, 'y', None)
    in_specs = (P(None, 'dp'), P('dp'), P(None, 'dp', None), P(None, 'x'), cache_spec, cache_spec, P('x'), P('x', 'y'), P('x', 'y'), P('x', 'y'), P('y', 'x'), P('x'), P('x', None), P(None, 'x', 'y'), P(None, 'x', 'y'), P(None, 'y', 'x'))
    out_specs = (P(None, 'dp', 'x'), cache_spec, cache_spec)

    def per_device(tokens, lengths, choices, emb_table, k_cache, v_cache, g_attn, w_q, w_k, w_v, w_o, g_ffn, w_router, w_act, w_lin, w_down):
        steps, nb = tokens.shape
        seq, kvl, hdim = k_cache.shape[1:]
        q_cols, kv_cols = w_q.shape[1], w_k.shape[1]
        width = emb_table.shape[1]
        width_full = width * x_count
        group = q_cols // kv_cols
        rows = steps * nb
        top = choices.shape[2]
        positions = (lengths[None, :] + jnp.arange(steps, dtype=lengths.dtype)[:, None]).reshape(rows)
        wq = w_q.reshape(width, kvl, group, hdim).transpose(0, 2, 1, 3).reshape(width, q_cols)
        wo = w_o.reshape(kvl, group, hdim, width).transpose(1, 0, 2, 3).reshape(q_cols, width)
        w_all = jnp.concatenate([wq, w_k, w_v], axis=1)
        chb = jnp.broadcast_to(choices.reshape(rows, top).T.astype(BF16)[:, :, None], (top, rows, LANE))
        wr = jnp.pad(w_router, ((0, 0), (0, LANE - w_router.shape[1])))

        cosv, sinv = turn_tables(positions, hdim)
        x_in = jnp.take(emb_table, tokens.reshape(rows), axis=0)
        gain_a, gain_f = g_attn.astype(F32).reshape(1, width), g_ffn.astype(F32).reshape(1, width)
        proj = front(x_in, gain_a, w_all, cosv.reshape(steps, nb, LANE), sinv.reshape(steps, nb, LANE), steps, width_full, q_cols + kv_cols)
        q = proj[:, :, :q_cols].reshape(steps, nb, group, kv_cols).transpose(1, 0, 2, 3).reshape(nb, steps * group, kv_cols)
        q = jnp.pad(q, ((0, 0), (0, QROWS - steps * group), (0, 0)))
        kn = proj[:, :, q_cols:q_cols + kv_cols].transpose(1, 0, 2).reshape(nb // NB, NB * steps, kv_cols)
        vn = proj[:, :, q_cols + kv_cols:].transpose(1, 0, 2).reshape(nb // NB, NB * steps, kv_cols)
        pad = -(NB * steps) % 32
        kn = jnp.pad(kn, ((0, 0), (0, pad), (0, 0)))
        vn = jnp.pad(vn, ((0, 0), (0, pad), (0, 0)))
        kc = k_cache.transpose(0, 2, 3, 1).reshape(nb, kv_cols, seq)
        vc = v_cache.transpose(0, 2, 3, 1).reshape(nb, kv_cols, seq)
        o, ko, vo = attention(lengths, q, kn, vn, kc, vc, steps, group)
        mixed = o[:, :steps * group].reshape(nb, steps, q_cols).transpose(1, 0, 2).reshape(rows, q_cols)
        hidden = tail(mixed, wo, x_in, gain_f, wr, chb, w_act, w_lin, w_down, steps, width_full)
        ko = ko.reshape(nb, kvl, hdim, seq).transpose(0, 3, 1, 2)
        vo = vo.reshape(nb, kvl, hdim, seq).transpose(0, 3, 1, 2)
        return hidden, ko, vo

    return jax.shard_map(per_device, mesh=mesh, in_specs=in_specs, out_specs=out_specs, check_vma=False)
```

```python
import functools
import jax
import jax.numpy as jnp
from jax import lax
from jax.experimental import pallas as pl
from jax.experimental.pallas import tpu as pltpu
from jax.sharding import PartitionSpec as P

EPS = 1e-5
ROPE_BASE = 1.0e6
MESH = pl.DeviceIdType.MESH
F32 = jnp.float32
BF16 = jnp.bfloat16
LANE = 128
SUB = 16
MIB = 1024 * 1024
LOWEST = -1.0e30
NB = 16
QROWS = 16
HEAD = 64
NEAR = 3


def attn_body(len_ref, q_ref, kn_ref, vn_ref, k_ref, v_ref, o_ref, ko_ref, vo_ref, s_ref, w_ref, qs, ks, vs, os_, *, group):
    half, seq = k_ref.shape[1:]
    steps, n_seq = q_ref.shape[:2]
    step = pl.program_id(0)

    @pl.when(step == 0)
    def _():
        for ref in (qs, ks, vs):
            ref[...] = jnp.zeros_like(ref)

    for t in range(steps):
        ks[pl.ds(t, n_seq, stride=steps), :] = kn_ref[t].astype(F32)
        vs[pl.ds(t, n_seq, stride=steps), :] = vn_ref[t].astype(F32)
        for g in range(group):
            qs[pl.ds(t * group + g, n_seq, stride=QROWS), :] = q_ref[t, :, LANE * g:LANE * (g + 1)].astype(F32)
    kn_t = ks[...].T
    vn_t = vs[...].T
    lane = lax.broadcasted_iota(jnp.int32, (SUB, LANE), 1).astype(F32).astype(BF16)
    srow = lax.broadcasted_iota(jnp.int32, (2 * QROWS, seq), 0)
    scol = lax.broadcasted_iota(jnp.int32, (2 * QROWS, seq), 1)
    srow = jnp.where(srow >= QROWS, srow - QROWS, srow)
    rel = scol - jnp.where(srow >= 2 * group, 2, jnp.where(srow >= group, 1, 0))
    low = lax.broadcasted_iota(jnp.int32, (QROWS, LANE), 1) < HEAD
    low_b = lane < jnp.asarray(HEAD, BF16)
    for b in range(n_seq):
        pos = len_ref[step * n_seq + b]
        turn = lax.rem(pos + LANE - b * steps, LANE)
        new = (pltpu.roll(kn_t, turn, 1).astype(BF16), pltpu.roll(vn_t, turn, 1).astype(BF16))
        gap = lane - jnp.full((SUB, LANE), pos.astype(F32), F32).astype(BF16)
        for tile in range(seq // LANE):
            lo = jnp.asarray(-LANE * tile, BF16)
            hi = jnp.asarray(steps - 1 - LANE * tile, BF16)
            hit = (gap >= lo) & (gap <= hi)
            for i in range(half // SUB):
                rs, cs = slice(SUB * i, SUB * i + SUB), slice(LANE * tile, LANE * tile + LANE)
                ko_ref[b, rs, cs] = jnp.where(hit, new[0][rs], k_ref[b, rs, cs])
                vo_ref[b, rs, cs] = jnp.where(hit, new[1][rs], v_ref[b, rs, cs])
    for b in range(n_seq):
        q16 = qs[QROWS * b:QROWS * (b + 1), :].astype(BF16)
        zero = jnp.zeros_like(q16)
        q32 = jnp.concatenate([jnp.where(low_b, q16, zero), jnp.where(low_b, zero, q16)], axis=0)
        s_ref[b] = jnp.dot(q32, ko_ref[b], preferred_element_type=F32)
    tots = []
    for b in range(n_seq):
        pos = len_ref[step * n_seq + b]
        ok = rel <= pos
        s = jnp.where(ok, s_ref[b] * HEAD ** -0.5, LOWEST)
        peak = jnp.max(s, axis=1, keepdims=True)
        w = jnp.where(ok, jnp.exp(s - peak), 0.0)
        tots.append(jnp.sum(w, axis=1, keepdims=True))
        w_ref[b] = w.astype(BF16)
    for b in range(n_seq):
        o = lax.dot_general(w_ref[b], vo_ref[b], (((1,), (1,)), ((), ())), preferred_element_type=F32)
        o = o / tots[b]
        os_[QROWS * b:QROWS * (b + 1), :] = jnp.where(low, o[:QROWS], o[QROWS:])
    for t in range(steps):
        og = [os_[pl.ds(t * group + g, n_seq, stride=QROWS), :] for g in range(group)]
        turned = pltpu.roll(og[1], HEAD, 1)
        first = low[:n_seq]
        tiles = (jnp.where(first, og[0], turned), jnp.where(first, og[2], og[0]), jnp.where(first, turned, og[2]))
        for g in range(group):
            o_ref[t, :, LANE * g:LANE * (g + 1)] = tiles[g].astype(BF16)


def attention(lengths, proj, kc, vc, group):
    nb, half, seq = kc.shape
    steps = proj.shape[0]
    cache = pl.BlockSpec((NB, half, seq), lambda i, l: (i, 0, 0))
    qs = pl.BlockSpec((steps, NB, group * LANE), lambda i, l: (0, i, 0))
    kspec = pl.BlockSpec((steps, NB, LANE), lambda i, l: (0, i, group))
    vspec = pl.BlockSpec((steps, NB, LANE), lambda i, l: (0, i, group + 1))
    flat = pltpu.VMEM((NB * QROWS, LANE), F32)
    new = pltpu.VMEM((LANE, LANE), F32)
    return pl.pallas_call(
        functools.partial(attn_body, group=group),
        grid_spec=pltpu.PrefetchScalarGridSpec(num_scalar_prefetch=1, grid=(nb // NB,), in_specs=[qs, kspec, vspec, cache, cache], out_specs=[qs, cache, cache],
            scratch_shapes=[pltpu.VMEM((NB, 2 * QROWS, seq), F32), pltpu.VMEM((NB, 2 * QROWS, seq), BF16), flat, new, new, flat]),
        out_shape=[jax.ShapeDtypeStruct((steps, nb, group * LANE), BF16), jax.ShapeDtypeStruct(kc.shape, BF16), jax.ShapeDtypeStruct(vc.shape, BF16)],
        compiler_params=pltpu.CompilerParams(vmem_limit_bytes=40 * MIB, dimension_semantics=("arbitrary",)),
        cost_estimate=pl.CostEstimate(flops=2 * nb * 32 * LANE * seq * 2, bytes_accessed=4 * nb * half * seq * 2, transcendentals=0),
    )(lengths, proj, proj, proj, kc, vc)


def remote(src, dst, ssem, rsem, dev):
    return pltpu.make_async_remote_copy(src_ref=src, dst_ref=dst, send_sem=ssem, recv_sem=rsem, device_id=dev, device_id_type=MESH)


def square_lanes(x_f32):
    acc = x_f32[:, 0:LANE] * x_f32[:, 0:LANE]
    for i in range(1, x_f32.shape[1] // LANE):
        part = x_f32[:, LANE * i:LANE * (i + 1)]
        acc = acc + part * part
    return acc


def square_rows(x_f32):
    return jnp.sum(square_lanes(x_f32).T, axis=0, keepdims=True)


def scale_rows(x_f32, stat_row, gain, width_full):
    scale = lax.rsqrt(stat_row / width_full + EPS)
    col = jnp.broadcast_to(scale, (LANE, LANE)).T
    parts = [x_f32[:, LANE * i:LANE * (i + 1)] * col * gain[:, LANE * i:LANE * (i + 1)] for i in range(x_f32.shape[1] // LANE)]
    return jnp.concatenate(parts, axis=1).astype(BF16)


def front_body(x_ref, g_ref, wq_ref, wk_ref, wv_ref, cos_ref, sin_ref, out_ref, st, st_in, hh, pj, rs1, cs, rs2, sts, str_, s1s, s1r, s2s, s2r, s3s, s3r, *, width_full):
    steps, nb = out_ref.shape[:2]
    q_cols, k_cols = wq_ref.shape[1], wk_ref.shape[1]
    gain = g_ref[0:1, :]
    cols = out_ref.shape[2]
    hb = nb // 2
    dp, y, x = lax.axis_index("dp"), lax.axis_index("y"), lax.axis_index("x")
    core, chip = x % 2, x // 2
    sib = (dp, y, chip * 2 + (1 - core))
    peer = (dp, y, (1 - chip) * 2 + core)
    diag = (dp, y, (1 - chip) * 2 + (1 - core))
    near = (sib, peer, diag)
    barrier = pltpu.get_barrier_semaphore()
    for dev in near:
        pl.semaphore_signal(barrier, inc=1, device_id=dev, device_id_type=MESH)
    keep = pl.multiple_of(core * hb, hb)
    give = pl.multiple_of((1 - core) * hb, hb)
    st[...] = jnp.zeros_like(st)
    blocks = steps * nb // LANE
    for i in range(blocks):
        st[i:i + 1, :] = square_rows(x_ref[LANE * i:LANE * (i + 1), :].astype(F32))
    pl.semaphore_wait(barrier, 3)
    stat = [remote(st, st_in.at[k], sts.at[k], str_.at[k], near[k]) for k in range(3)]
    for k in range(3):
        stat[k].start()
    for k in range(3):
        stat[k].wait_recv()
    total = st[...] + st_in[0] + st_in[1] + st_in[2]

    def s1(c):
        return remote(pj.at[c, pl.ds(give, hb), :], rs1.at[c], s1s.at[c], s1r.at[c], sib)

    def s2(c):
        return remote(cs.at[c], rs2.at[c], s2s.at[c], s2r.at[c], peer)

    def s3(c, row):
        return remote(out_ref.at[c, pl.ds(row, hb), :], out_ref.at[c, pl.ds(row, hb), :], s3s.at[c], s3r.at[c], sib)

    def mid(c):
        s1(c).wait_recv()
        cs[c] = (pj[c, pl.ds(keep, hb), :].astype(F32) + rs1[c].astype(F32)).astype(BF16)
        s2(c).start()

    def last(c):
        s2(c).wait_recv()
        fin = (cs[c].astype(F32) + rs2[c].astype(F32)).astype(BF16).astype(F32)
        cosv = cos_ref[c, pl.ds(keep, hb), :]
        sinv = sin_ref[c, pl.ds(keep, hb), :]
        lane = lax.broadcasted_iota(jnp.int32, (hb, LANE), 1)
        first, low = lane % HEAD < HEAD // 2, lane < HEAD
        tiles = [fin[:, LANE * i:LANE * (i + 1)] for i in range(cols // LANE)]
        for i in range((q_cols + k_cols) // LANE):
            v = tiles[i]
            swap = jnp.where(first, pltpu.roll(v, LANE - HEAD // 2, 1), pltpu.roll(v, HEAD // 2, 1))
            tiles[i] = v * cosv + swap * sinv
        ta, tb, tc = tiles[:NEAR]
        tiles[:NEAR] = [jnp.where(low, ta, tb), pltpu.roll(jnp.where(low, tc, ta), HEAD, 1), jnp.where(low, tb, tc)]
        for i in range(cols // LANE):
            out_ref[c, pl.ds(keep, hb), LANE * i:LANE * (i + 1)] = tiles[i].astype(BF16)
        s3(c, keep).start()

    for c in range(steps):
        for i in range(c * nb // LANE, (c + 1) * nb // LANE):
            hh[LANE * i:LANE * (i + 1), :] = scale_rows(x_ref[LANE * i:LANE * (i + 1), :].astype(F32), total[i:i + 1, :], gain, width_full)
        normed = hh[c * nb:(c + 1) * nb, :]
        pj[c, :, 0:q_cols] = jnp.dot(normed, wq_ref[...], preferred_element_type=F32).astype(BF16)
        pj[c, :, q_cols:q_cols + k_cols] = jnp.dot(normed, wk_ref[...], preferred_element_type=F32).astype(BF16)
        pj[c, :, q_cols + k_cols:cols] = jnp.dot(normed, wv_ref[...], preferred_element_type=F32).astype(BF16)
        s1(c).start()
        if c >= 1:
            mid(c - 1)
    mid(steps - 1)
    for c in range(steps):
        last(c)
    for c in range(steps):
        s3(c, give).wait_recv()
    for k in range(3):
        stat[k].wait_send()
    for c in range(steps):
        s1(c).wait_send()
        s2(c).wait_send()
        s3(c, keep).wait_send()


def front(x_in, gain, w_q, w_k, w_v, cosv, sinv, steps, width_full):
    rows, width = x_in.shape
    nb = rows // steps
    cols = w_q.shape[1] + 2 * w_k.shape[1]
    hb = nb // 2
    dma = pltpu.SemaphoreType.DMA
    vm = pl.BlockSpec(memory_space=pltpu.VMEM)
    return pl.pallas_call(
        functools.partial(front_body, width_full=width_full),
        out_shape=jax.ShapeDtypeStruct((steps, nb, cols), BF16),
        in_specs=[vm] * 7,
        out_specs=vm,
        scratch_shapes=[
            pltpu.VMEM((8, LANE), F32), pltpu.VMEM((3, 8, LANE), F32),
            pltpu.VMEM((rows, width), BF16), pltpu.VMEM((steps, nb, cols), BF16),
            pltpu.VMEM((steps, hb, cols), BF16), pltpu.VMEM((steps, hb, cols), BF16), pltpu.VMEM((steps, hb, cols), BF16),
            dma((3,)), dma((3,)), dma((steps,)), dma((steps,)), dma((steps,)), dma((steps,)), dma((steps,)), dma((steps,)),
        ],
        compiler_params=pltpu.CompilerParams(collective_id=2, has_side_effects=True, vmem_limit_bytes=24 * MIB),
        cost_estimate=pl.CostEstimate(flops=2 * rows * width * cols, bytes_accessed=4 * MIB, transcendentals=0),
    )(x_in, gain, w_q, w_k, w_v, cosv, sinv)


def tail_body(mix_ref, wo_ref, xin_ref, g_ref, wr_ref, ch_ref, wact_hbm, wlin_hbm, wdn_hbm, out_ref,
              wcat, wdn, pa, ar, xm, hh, st, st_in, hs, rs1, cs, rs2, lgp, lr1, lcs, lr2, u, pd, yr,
              wsem, as_, ar_s, xs, xr, sts, str_, s1s, s1r, s2s, s2r, l1s, l1r, l2s, l2r, us, ur, ys, yrs, gs, gr, *, width_full):
    experts = wcat.shape[0]
    ff = wact_hbm.shape[2]
    steps, top, nb = ch_ref.shape
    parts = rs1.shape[0]
    per = parts // steps
    ns = nb // per
    hb, qb = ns // 2, ns // 4
    dp, y, x = lax.axis_index("dp"), lax.axis_index("y"), lax.axis_index("x")
    core, chip = x % 2, x // 2
    sib = (dp, y, chip * 2 + (1 - core))
    peer = (dp, y, (1 - chip) * 2 + core)
    diag = (dp, y, (1 - chip) * 2 + (1 - core))
    near = (sib, peer, diag)
    hops = range(1, NEAR + 1)
    ypeer = [None] + [(dp, (y + d) % (NEAR + 1), x) for d in hops]
    slots = range(NEAR)
    nothing = (((1,), (1,)), ((), ()))

    w0 = pltpu.make_async_copy(wact_hbm, wcat.at[:, :, pl.ds(0, ff)], wsem.at[0])
    w1 = pltpu.make_async_copy(wlin_hbm, wcat.at[:, :, pl.ds(ff, ff)], wsem.at[1])
    w2 = pltpu.make_async_copy(wdn_hbm, wdn, wsem.at[2])
    barrier = pltpu.get_barrier_semaphore()
    for dev in near + tuple(ypeer[1:]):
        pl.semaphore_signal(barrier, inc=1, device_id=dev, device_id_type=MESH)

    def rows(k, start, size):
        return pl.ds(pl.multiple_of(k * ns + start, SUB), size)

    keep, give = core * hb, (1 - core) * hb
    sub_keep, sub_give = chip * qb, (1 - chip) * qb
    own, other = keep + sub_keep, keep + sub_give
    sib_own, sib_other = give + sub_keep, give + sub_give

    def ydist(d):
        return ((y + d) % (NEAR + 1)) * qb

    def rs_send(buf, land, ssem, rsem, k, d):
        return remote(buf.at[rows(k, ydist(d), qb), :], land.at[k, NEAR - d], ssem.at[k, d - 1], rsem.at[k, NEAR - d], ypeer[d])

    def rs_recv(buf, land, ssem, rsem, k, i):
        return remote(buf.at[rows(k, 0, qb), :], land.at[k, i], ssem.at[k, i], rsem.at[k, i], ypeer[1])

    def ag_send(buf, ssem, rsem, k, d):
        mine = buf.at[rows(k, y * qb, qb), :]
        return remote(mine, mine, ssem.at[k, d - 1], rsem.at[k, NEAR - d], ypeer[d])

    def ag_recv(buf, ssem, rsem, k, i):
        theirs = buf.at[rows(k, ydist(i + 1), qb), :]
        return remote(theirs, theirs, ssem.at[k, i], rsem.at[k, i], ypeer[1])

    def s1(k):
        return remote(hs.at[rows(k, give, hb), :], rs1.at[k], s1s.at[k], s1r.at[k], sib)

    def s2(k):
        return remote(cs.at[k], rs2.at[k], s2s.at[k], s2r.at[k], peer)

    def l1(k):
        return remote(lgp.at[rows(k, give, hb), :], lr1.at[k], l1s.at[k], l1r.at[k], sib)

    def l2(k):
        return remote(lcs.at[k], lr2.at[k], l2s.at[k], l2r.at[k], peer)

    def u_copy(k, row, i):
        blk = u.at[rows(k, row, qb), :]
        return remote(blk, blk, us.at[k, i], ur.at[k, i], peer if i == 0 else sib)

    def stat(k, i):
        return remote(st.at[k], st_in.at[k, i], sts.at[k, i], str_.at[k, i], near[i])

    def attn_out(c):
        pa[c * nb:(c + 1) * nb, :] = jnp.dot(mix_ref[c], wo_ref[...], preferred_element_type=F32).astype(BF16)

    def attn_send(k):
        for d in hops:
            rs_send(pa, ar, as_, ar_s, k, d).start()

    def attn_sum(k):
        for i in slots:
            rs_recv(pa, ar, as_, ar_s, k, i).wait_recv()
        acc = pa[rows(k, y * qb, qb), :].astype(F32)
        for i in slots:
            acc = acc + ar[k, i].astype(F32)
        mid = (xin_ref[rows(k, y * qb, qb), :].astype(F32) + acc).astype(BF16)
        xm[k] = mid
        st[k] = square_lanes(mid.astype(F32))
        for i in slots:
            stat(k, i).start()

    def norm(k):
        for i in slots:
            stat(k, i).wait_recv()
        total = st[k]
        for i in slots:
            total = total + st_in[k, i]
        scale = lax.rsqrt(jnp.sum(total, axis=1, keepdims=True) / width_full + EPS)
        hh[rows(k, y * qb, qb), :] = (xm[k].astype(F32) * scale * g_ref[1:2, :]).astype(BF16)
        for d in hops:
            ag_send(hh, xs, xr, k, d).start()

    def ready(c):
        for k in range(c * per, (c + 1) * per):
            for i in slots:
                ag_recv(hh, xs, xr, k, i).wait_recv()
        blk = slice(c * nb, (c + 1) * nb)
        lgp[blk, 0:experts] = lax.dot_general(hh[blk, :], wr_ref[...], nothing, preferred_element_type=F32)
        for k in range(c * per, (c + 1) * per):
            l1(k).start()

    def experts_in(c, part, hd):
        span = 4
        half = experts // span // 2

        def few(i, carry):
            for q in range(span):
                e = i * span + q
                hval = jnp.dot(hh[c * nb:(c + 1) * nb, :], wcat[e], preferred_element_type=F32)
                hd[e] = hval[:, 0:ff].astype(BF16)
                hd[experts + e] = hval[:, ff:2 * ff].astype(BF16)
            return carry
        lax.fori_loop(part * half, (part + 1) * half, few, 0)

    def pick(k, hd, chs):
        def tile(i, carry):
            r = pl.multiple_of((k % per) * ns + i * SUB, SUB)
            ch = [chs[j, rows(k, i * SUB, SUB), :] for j in range(top)]
            span = 8

            def some(g, state):
                acc, ev = list(state[0]), state[1]
                for q in range(span):
                    e = g * span + q
                    va = hd[e, pl.ds(r, SUB), :]
                    vl = hd[experts + e, pl.ds(r, SUB), :]
                    for j in range(top):
                        m = ch[j] == ev
                        acc[2 * j] = jnp.where(m, va, acc[2 * j])
                        acc[2 * j + 1] = jnp.where(m, vl, acc[2 * j + 1])
                    ev = ev + jnp.ones_like(ev)
                return tuple(acc), ev
            zero = jnp.zeros((SUB, ff), BF16)
            acc, _ = lax.fori_loop(0, experts // span, some, (tuple(zero for _ in range(2 * top)), zero))
            for q in range(2 * top):
                hs[rows(k, i * SUB, SUB), q * ff:(q + 1) * ff] = acc[q]
            return carry
        lax.fori_loop(0, ns // SUB, tile, 0)
        s1(k).start()

    def logits_mid(k):
        l1(k).wait_recv()
        lcs[k] = lgp[rows(k, other, qb), :] + lr1[k, pl.ds(pl.multiple_of(sub_give, SUB), qb), :]
        l2(k).start()

    def part_b(k):
        logits_mid(k)
        s1(k).wait_recv()

        def add(i, carry):
            mine = hs[rows(k, other + i * SUB, SUB), :].astype(F32)
            got = rs1[k, pl.ds(pl.multiple_of(sub_give + i * SUB, SUB), SUB), :].astype(F32)
            cs[k, pl.ds(pl.multiple_of(i * SUB, SUB), SUB), :] = (mine + got).astype(BF16)
            return carry
        lax.fori_loop(0, qb // SUB, add, 0)
        s2(k).start()

    def part_u(k, chs):
        l2(k).wait_recv()
        s2(k).wait_recv()

        def tile(i, carry):
            r = pl.ds(pl.multiple_of(i * SUB, SUB), SUB)
            r_own = rows(k, own + i * SUB, SUB)
            r_sub = pl.ds(pl.multiple_of(sub_keep + i * SUB, SUB), SUB)
            logit = lgp[r_own, :] + lr1[k, r_sub, :] + lr2[k, r, :]
            lane = lax.broadcasted_iota(jnp.int32, (SUB, LANE), 1).astype(F32)
            hit = [chs[j, r_own, :].astype(F32) == lane for j in range(top)]
            any_hit = hit[0]
            for j in range(1, top):
                any_hit = any_hit | hit[j]
            peak = jnp.max(jnp.where(any_hit, logit, -jnp.inf), axis=1, keepdims=True)
            ex = jnp.where(any_hit, jnp.exp(logit - peak), 0.0)
            coef = ex / jnp.sum(ex, axis=1, keepdims=True)
            for j in range(top):
                gate = jnp.sum(jnp.where(hit[j], coef, 0.0), axis=1, keepdims=True)
                ca, cl = pl.ds(2 * j * ff, ff), pl.ds((2 * j + 1) * ff, ff)
                act = hs[r_own, ca].astype(F32) + rs1[k, r_sub, ca].astype(F32) + rs2[k, r, ca].astype(F32)
                lin = hs[r_own, cl].astype(F32) + rs1[k, r_sub, cl].astype(F32) + rs2[k, r, cl].astype(F32)
                val = gate * (act / (1.0 + jnp.exp(-act))) * lin
                u[r_own, j * ff:(j + 1) * ff] = val.astype(BF16)
            return carry
        lax.fori_loop(0, qb // SUB, tile, 0)
        u_copy(k, own, 0).start()
        u_copy(k, own, 1).start()

    def part_f(k):
        u_copy(k, other, 0).wait_recv()
        u_copy(k, other, 2).start()

    def part_d(k, ud, chs, us16):
        u_copy(k, sib_own, 1).wait_recv()
        u_copy(k, sib_other, 2).wait_recv()
        for j in range(top):
            us16[j] = u[k * ns:(k + 1) * ns, j * ff:(j + 1) * ff]

        def spread(i, carry):
            r = pl.ds(pl.multiple_of(i * SUB, SUB), SUB)
            ch = [chs[j, rows(k, i * SUB, SUB), :] for j in range(top)]
            vals = [us16[j, r, :] for j in range(top)]
            for e in range(experts):
                acc = jnp.zeros((SUB, ff), BF16)
                for j in range(top):
                    acc = jnp.where(ch[j] == jnp.asarray(e, BF16), vals[j], acc)
                ud[r, e * ff:(e + 1) * ff] = acc
            return carry
        lax.fori_loop(0, ns // SUB, spread, 0)
        pd[k * ns:(k + 1) * ns, :] = jnp.dot(ud[...], wdn[...], preferred_element_type=F32).astype(BF16)
        for d in hops:
            rs_send(pd, yr, ys, yrs, k, d).start()

    def part_g(k):
        for i in slots:
            rs_recv(pd, yr, ys, yrs, k, i).wait_recv()
        acc = pd[rows(k, y * qb, qb), :].astype(F32)
        for i in slots:
            acc = acc + yr[k, i].astype(F32)
        out_ref[rows(k, y * qb, qb), :] = (xm[k].astype(F32) + acc).astype(BF16)
        for d in hops:
            ag_send(out_ref, gs, gr, k, d).start()

    def run(hd, ud, chs, us16):
        w0.start()
        w1.start()
        w2.start()
        for c in range(steps):
            attn_out(c)
        lgp[...] = jnp.zeros_like(lgp)
        for c in range(steps):
            for i in range(nb // LANE):
                for j in range(top):
                    row = ch_ref[c, j:j + 1, LANE * i:LANE * (i + 1)].astype(F32)
                    chs[j, c * nb + LANE * i:c * nb + LANE * (i + 1), :] = jnp.broadcast_to(row, (LANE, LANE)).T.astype(BF16)
        pl.semaphore_wait(barrier, 2 * NEAR)
        attn_send(0)
        attn_send(1)
        attn_sum(0)
        attn_sum(1)
        norm(0)
        norm(1)
        attn_send(2)
        attn_send(3)
        ready(0)
        w0.wait()
        w1.wait()
        experts_in(0, 0, hd)
        attn_sum(2)
        attn_sum(3)
        experts_in(0, 1, hd)
        norm(2)
        norm(3)
        attn_send(4)
        attn_send(5)
        pick(0, hd, chs)
        pick(1, hd, chs)
        part_b(0)
        part_b(1)
        ready(1)
        experts_in(1, 0, hd)
        attn_sum(4)
        attn_sum(5)
        experts_in(1, 1, hd)
        norm(4)
        norm(5)
        part_u(0, chs)
        pick(2, hd, chs)
        part_u(1, chs)
        pick(3, hd, chs)
        part_b(2)
        part_f(0)
        part_b(3)
        part_f(1)
        w2.wait()
        part_d(0, ud, chs, us16)
        ready(2)
        experts_in(2, 0, hd)
        part_d(1, ud, chs, us16)
        experts_in(2, 1, hd)
        part_u(2, chs)
        pick(4, hd, chs)
        part_u(3, chs)
        pick(5, hd, chs)
        part_b(4)
        part_f(2)
        part_b(5)
        part_f(3)
        part_g(0)
        part_d(2, ud, chs, us16)
        part_g(1)
        part_u(4, chs)
        part_d(3, ud, chs, us16)
        part_u(5, chs)
        part_f(4)
        part_g(2)
        part_d(4, ud, chs, us16)
        part_f(5)
        part_g(3)
        part_d(5, ud, chs, us16)
        part_g(4)
        part_g(5)

    bf = functools.partial(pltpu.VMEM, dtype=BF16)
    pl.run_scoped(run, bf((2 * experts, nb, ff)), bf((ns, experts * ff)), bf((top, steps * nb, ff)), bf((top, ns, ff)))

    for k in range(parts):
        for i in slots:
            ag_recv(out_ref, gs, gr, k, i).wait_recv()
    for k in range(parts):
        for i in slots:
            stat(k, i).wait_send()
        l1(k).wait_send()
        l2(k).wait_send()
        s1(k).wait_send()
        s2(k).wait_send()
        u_copy(k, own, 0).wait_send()
        u_copy(k, own, 1).wait_send()
        u_copy(k, other, 2).wait_send()
        for d in hops:
            rs_send(pa, ar, as_, ar_s, k, d).wait_send()
            ag_send(hh, xs, xr, k, d).wait_send()
            rs_send(pd, yr, ys, yrs, k, d).wait_send()
            ag_send(out_ref, gs, gr, k, d).wait_send()


def tail(mixed, wo, x_in, gain, w_router, chosen, w_act, w_lin, w_down, width_full):
    total, width = x_in.shape
    steps, top, nb = chosen.shape
    experts, _, ff = w_act.shape
    parts = 2 * steps
    ns = nb // 2
    hb, qb = ns // 2, ns // 4
    dma = pltpu.SemaphoreType.DMA
    vm = pl.BlockSpec(memory_space=pltpu.VMEM)
    hbm = pl.BlockSpec(memory_space=pl.ANY)
    bf = functools.partial(pltpu.VMEM, dtype=BF16)
    fl = functools.partial(pltpu.VMEM, dtype=F32)
    wide = 2 * top * ff
    each, three = (parts,), (parts, NEAR)
    sems = [three] * 6 + [each] * 8 + [three] * 6
    return pl.pallas_call(
        functools.partial(tail_body, width_full=width_full),
        out_shape=jax.ShapeDtypeStruct((total, width), BF16),
        in_specs=[vm] * 6 + [hbm] * 3,
        out_specs=vm,
        scratch_shapes=[
            bf((experts, width, 2 * ff)), bf((experts * ff, width)),
            bf((total, width)), bf((parts, NEAR, qb, width)), bf((parts, qb, width)), bf((total, width)),
            fl((parts, qb, LANE)), fl((parts, NEAR, qb, LANE)),
            bf((total, wide)), bf((parts, hb, wide)), bf((parts, qb, wide)), bf((parts, qb, wide)),
            fl((total, LANE)), fl((parts, hb, LANE)), fl((parts, qb, LANE)), fl((parts, qb, LANE)),
            bf((total, top * ff)), bf((total, width)), bf((parts, NEAR, qb, width)),
            dma((NEAR,)),
        ] + [dma(n) for n in sems],
        compiler_params=pltpu.CompilerParams(collective_id=1, has_side_effects=True, vmem_limit_bytes=60 * MIB),
        cost_estimate=pl.CostEstimate(flops=6 * total * width * experts * ff, bytes_accessed=12 * MIB, transcendentals=0),
    )(mixed, wo, x_in, gain, w_router, chosen, w_act, w_lin, w_down.reshape(experts * ff, width))


def turn_tables(positions, head_dim):
    half_dim = head_dim // 2
    inv_freq = ROPE_BASE ** (-(jnp.arange(half_dim, dtype=F32) * 2.0 / head_dim))
    angles = positions.astype(F32)[:, None] * inv_freq[None, :]
    cosine, sine_val = jnp.cos(angles), jnp.sin(angles)
    return jnp.tile(cosine, (1, 4)), jnp.tile(jnp.concatenate([-sine_val, sine_val], axis=1), (1, 2))


def solution(mesh):
    x_count = mesh.shape['x']
    cache_spec = P('dp', None, 'y', None)
    in_specs = (P(None, 'dp'), P('dp'), P(None, 'dp', None), P(None, 'x'), cache_spec, cache_spec, P('x'), P('x', 'y'), P('x', 'y'), P('x', 'y'), P('y', 'x'), P('x'), P('x', None), P(None, 'x', 'y'), P(None, 'x', 'y'), P(None, 'y', 'x'))
    out_specs = (P(None, 'dp', 'x'), cache_spec, cache_spec)

    def per_device(tokens, lengths, choices, emb_table, k_cache, v_cache, g_attn, w_q, w_k, w_v, w_o, g_ffn, w_router, w_act, w_lin, w_down):
        steps, nb = tokens.shape
        seq, kvl, hdim = k_cache.shape[1:]
        q_cols, kv_cols = w_q.shape[1], w_k.shape[1]
        width = emb_table.shape[1]
        width_full = width * x_count
        group = q_cols // kv_cols
        rows = steps * nb
        positions = (lengths[None, :] + jnp.arange(steps, dtype=lengths.dtype)[:, None]).reshape(rows)
        cosv, sinv = turn_tables(positions, hdim)
        x_in = emb_table.at[tokens].get(mode="promise_in_bounds").reshape(rows, width)
        first = lax.broadcasted_iota(jnp.int32, (2, width), 0) == 0
        gains = jnp.where(first, g_attn[None, :], g_ffn[None, :]).astype(F32)
        proj = front(x_in, gains, w_q, w_k, w_v, cosv.reshape(steps, nb, LANE), sinv.reshape(steps, nb, LANE), steps, width_full)
        kc = k_cache.transpose(0, 2, 3, 1).reshape(nb, kv_cols, seq)
        vc = v_cache.transpose(0, 2, 3, 1).reshape(nb, kv_cols, seq)
        mixed, ko, vo = attention(lengths, proj, kc, vc, group)
        hidden = tail(mixed, w_o, x_in, gains, w_router.T, choices.transpose(0, 2, 1), w_act, w_lin, w_down, width_full).reshape(steps, nb, width)
        ko = ko.reshape(nb, kvl, hdim, seq).transpose(0, 3, 1, 2)
        vo = vo.reshape(nb, kvl, hdim, seq).transpose(0, 3, 1, 2)
        return hidden, ko, vo

    return jax.shard_map(per_device, mesh=mesh, in_specs=in_specs, out_specs=out_specs, check_vma=False)
```

```python
import functools
import jax
import jax.numpy as jnp
from jax import lax
from jax.experimental import pallas as pl
from jax.experimental.pallas import tpu as pltpu
from jax.sharding import PartitionSpec as P

EPS = 1e-5
ROPE_BASE = 1.0e6
MESH = pl.DeviceIdType.MESH
F32 = jnp.float32
BF16 = jnp.bfloat16
LANE = 128
SUB = 16
MIB = 1024 * 1024
LOWEST = -1.0e30
NB = 32
QROWS = 16
HEAD = 64
NEAR = 3


def attn_body(len_ref, q_ref, kn_ref, vn_ref, k_ref, v_ref, o_ref, ko_ref, vo_ref, s_ref, w_ref, qs, ks, vs, os_, *, group):
    half, seq = k_ref.shape[1:]
    steps, n_seq = q_ref.shape[:2]
    step = pl.program_id(0)

    @pl.when(step == 0)
    def _():
        for ref in (qs, ks, vs):
            ref[...] = jnp.zeros_like(ref)

    for t in range(steps):
        ks[pl.ds(t, n_seq, stride=steps), :] = kn_ref[t].astype(F32)
        vs[pl.ds(t, n_seq, stride=steps), :] = vn_ref[t].astype(F32)
        for g in range(group):
            qs[pl.ds(t * group + g, n_seq, stride=QROWS), :] = q_ref[t, :, LANE * g:LANE * (g + 1)].astype(F32)
    kn_t = ks[...].T
    vn_t = vs[...].T
    lane = lax.broadcasted_iota(jnp.int32, (SUB, LANE), 1).astype(F32).astype(BF16)
    srow = lax.broadcasted_iota(jnp.int32, (2 * QROWS, seq), 0)
    scol = lax.broadcasted_iota(jnp.int32, (2 * QROWS, seq), 1)
    srow = jnp.where(srow >= QROWS, srow - QROWS, srow)
    rel = scol - jnp.where(srow >= 2 * group, 2, jnp.where(srow >= group, 1, 0))
    low = lax.broadcasted_iota(jnp.int32, (QROWS, LANE), 1) < HEAD
    low_b = lane < jnp.asarray(HEAD, BF16)
    for b in range(n_seq):
        pos = len_ref[step * n_seq + b]
        turn = lax.rem(pos + LANE - b * steps, LANE)
        new = (pltpu.roll(kn_t, turn, 1).astype(BF16), pltpu.roll(vn_t, turn, 1).astype(BF16))
        gap = lane - jnp.full((SUB, LANE), pos.astype(F32), F32).astype(BF16)
        for tile in range(seq // LANE):
            lo = jnp.asarray(-LANE * tile, BF16)
            hi = jnp.asarray(steps - 1 - LANE * tile, BF16)
            hit = (gap >= lo) & (gap <= hi)
            for i in range(half // SUB):
                rs, cs = slice(SUB * i, SUB * i + SUB), slice(LANE * tile, LANE * tile + LANE)
                ko_ref[b, rs, cs] = jnp.where(hit, new[0][rs], k_ref[b, rs, cs])
                vo_ref[b, rs, cs] = jnp.where(hit, new[1][rs], v_ref[b, rs, cs])
    for b in range(n_seq):
        q16 = qs[QROWS * b:QROWS * (b + 1), :].astype(BF16)
        zero = jnp.zeros_like(q16)
        q32 = jnp.concatenate([jnp.where(low_b, q16, zero), jnp.where(low_b, zero, q16)], axis=0)
        s_ref[b] = jnp.dot(q32, ko_ref[b], preferred_element_type=F32)
    tots = []
    for b in range(n_seq):
        pos = len_ref[step * n_seq + b]
        ok = rel <= pos
        s = jnp.where(ok, s_ref[b] * HEAD ** -0.5, LOWEST)
        peak = jnp.max(s, axis=1, keepdims=True)
        w = jnp.where(ok, jnp.exp(s - peak), 0.0)
        tots.append(jnp.sum(w, axis=1, keepdims=True))
        w_ref[b] = w.astype(BF16)
    for b in range(n_seq):
        o = lax.dot_general(w_ref[b], vo_ref[b], (((1,), (1,)), ((), ())), preferred_element_type=F32)
        o = o / tots[b]
        os_[QROWS * b:QROWS * (b + 1), :] = jnp.where(low, o[:QROWS], o[QROWS:])
    for t in range(steps):
        og = [os_[pl.ds(t * group + g, n_seq, stride=QROWS), :] for g in range(group)]
        turned = pltpu.roll(og[1], HEAD, 1)
        first = lax.broadcasted_iota(jnp.int32, (n_seq, LANE), 1) < HEAD
        tiles = (jnp.where(first, og[0], turned), jnp.where(first, og[2], og[0]), jnp.where(first, turned, og[2]))
        for g in range(group):
            o_ref[t, :, LANE * g:LANE * (g + 1)] = tiles[g].astype(BF16)


def attention(lengths, proj, kc, vc, group):
    nb, half, seq = kc.shape
    steps = proj.shape[0]
    cache = pl.BlockSpec((NB, half, seq), lambda i, l: (i, 0, 0))
    qs = pl.BlockSpec((steps, NB, group * LANE), lambda i, l: (0, i, 0))
    kspec = pl.BlockSpec((steps, NB, LANE), lambda i, l: (0, i, group))
    vspec = pl.BlockSpec((steps, NB, LANE), lambda i, l: (0, i, group + 1))
    flat = pltpu.VMEM((NB * QROWS, LANE), F32)
    new = pltpu.VMEM((LANE, LANE), F32)
    return pl.pallas_call(
        functools.partial(attn_body, group=group),
        grid_spec=pltpu.PrefetchScalarGridSpec(num_scalar_prefetch=1, grid=(nb // NB,), in_specs=[qs, kspec, vspec, cache, cache], out_specs=[qs, cache, cache],
            scratch_shapes=[pltpu.VMEM((NB, 2 * QROWS, seq), F32), pltpu.VMEM((NB, 2 * QROWS, seq), BF16), flat, new, new, flat]),
        out_shape=[jax.ShapeDtypeStruct((steps, nb, group * LANE), BF16), jax.ShapeDtypeStruct(kc.shape, BF16), jax.ShapeDtypeStruct(vc.shape, BF16)],
        compiler_params=pltpu.CompilerParams(vmem_limit_bytes=60 * MIB, dimension_semantics=("arbitrary",)),
        cost_estimate=pl.CostEstimate(flops=2 * nb * 32 * LANE * seq * 2, bytes_accessed=4 * nb * half * seq * 2, transcendentals=0),
    )(lengths, proj, proj, proj, kc, vc)


def remote(src, dst, ssem, rsem, dev):
    return pltpu.make_async_remote_copy(src_ref=src, dst_ref=dst, send_sem=ssem, recv_sem=rsem, device_id=dev, device_id_type=MESH)


def square_lanes(x_f32):
    acc = x_f32[:, 0:LANE] * x_f32[:, 0:LANE]
    for i in range(1, x_f32.shape[1] // LANE):
        part = x_f32[:, LANE * i:LANE * (i + 1)]
        acc = acc + part * part
    return acc


def square_rows(x_f32):
    return jnp.sum(square_lanes(x_f32).T, axis=0, keepdims=True)


def scale_rows(x_f32, stat_row, gain, width_full):
    scale = lax.rsqrt(stat_row / width_full + EPS)
    col = jnp.broadcast_to(scale, (LANE, LANE)).T
    parts = [x_f32[:, LANE * i:LANE * (i + 1)] * col * gain[:, LANE * i:LANE * (i + 1)] for i in range(x_f32.shape[1] // LANE)]
    return jnp.concatenate(parts, axis=1).astype(BF16)


def front_body(x_ref, g_ref, wq_ref, wk_ref, wv_ref, out_ref, st, st_in, hh, pj, rs1, cs, rs2, sts, str_, s1s, s1r, s2s, s2r, s3s, s3r, *, width_full):
    steps, nb = out_ref.shape[:2]
    q_cols, k_cols = wq_ref.shape[1], wk_ref.shape[1]
    gain = g_ref[0:1, :]
    cols = out_ref.shape[2]
    hb = nb // 2
    dp, y, x = lax.axis_index("dp"), lax.axis_index("y"), lax.axis_index("x")
    core, chip = x % 2, x // 2
    sib = (dp, y, chip * 2 + (1 - core))
    peer = (dp, y, (1 - chip) * 2 + core)
    diag = (dp, y, (1 - chip) * 2 + (1 - core))
    near = (sib, peer, diag)
    barrier = pltpu.get_barrier_semaphore()
    for dev in near:
        pl.semaphore_signal(barrier, inc=1, device_id=dev, device_id_type=MESH)
    keep = pl.multiple_of(core * hb, hb)
    give = pl.multiple_of((1 - core) * hb, hb)
    st[...] = jnp.zeros_like(st)
    blocks = steps * nb // LANE
    for i in range(blocks):
        st[i:i + 1, :] = square_rows(x_ref[LANE * i:LANE * (i + 1), :].astype(F32))
    pl.semaphore_wait(barrier, 3)
    stat = [remote(st, st_in.at[k], sts.at[k], str_.at[k], near[k]) for k in range(3)]
    for k in range(3):
        stat[k].start()
    for k in range(3):
        stat[k].wait_recv()
    total = st[...] + st_in[0] + st_in[1] + st_in[2]

    def s1(c):
        return remote(pj.at[c, pl.ds(give, hb), :], rs1.at[c], s1s.at[c], s1r.at[c], sib)

    def s2(c):
        return remote(cs.at[c], rs2.at[c], s2s.at[c], s2r.at[c], peer)

    def s3(c, row):
        return remote(out_ref.at[c, pl.ds(row, hb), :], out_ref.at[c, pl.ds(row, hb), :], s3s.at[c], s3r.at[c], sib)

    def mid(c):
        s1(c).wait_recv()
        cs[c] = (pj[c, pl.ds(keep, hb), :].astype(F32) + rs1[c].astype(F32)).astype(BF16)
        s2(c).start()

    def last(c):
        lane = lax.broadcasted_iota(jnp.int32, (hb, LANE), 1)
        inv_freq = ROPE_BASE ** (-((lane % (HEAD // 2)).astype(F32) * 2.0 / HEAD))
        length = jnp.broadcast_to(g_ref[2:3, pl.ds(keep, hb)], (LANE, hb)).T
        angle = (length + float(c)) * inv_freq
        first, low = lane % HEAD < HEAD // 2, lane < HEAD
        cosv, sinv = jnp.cos(angle), jnp.sin(angle)
        sinv = jnp.where(first, -sinv, sinv)
        s2(c).wait_recv()
        fin = (cs[c].astype(F32) + rs2[c].astype(F32)).astype(BF16).astype(F32)
        tiles = [fin[:, LANE * i:LANE * (i + 1)] for i in range(cols // LANE)]
        for i in range((q_cols + k_cols) // LANE):
            v = tiles[i]
            swap = jnp.where(first, pltpu.roll(v, LANE - HEAD // 2, 1), pltpu.roll(v, HEAD // 2, 1))
            tiles[i] = v * cosv + swap * sinv
        ta, tb, tc = tiles[:NEAR]
        tiles[:NEAR] = [jnp.where(low, ta, tb), pltpu.roll(jnp.where(low, tc, ta), HEAD, 1), jnp.where(low, tb, tc)]
        for i in range(cols // LANE):
            out_ref[c, pl.ds(keep, hb), LANE * i:LANE * (i + 1)] = tiles[i].astype(BF16)
        s3(c, keep).start()

    for c in range(steps):
        for i in range(c * nb // LANE, (c + 1) * nb // LANE):
            hh[LANE * i:LANE * (i + 1), :] = scale_rows(x_ref[LANE * i:LANE * (i + 1), :].astype(F32), total[i:i + 1, :], gain, width_full)
        normed = hh[c * nb:(c + 1) * nb, :]
        pj[c, :, 0:q_cols] = jnp.dot(normed, wq_ref[...], preferred_element_type=F32).astype(BF16)
        pj[c, :, q_cols:q_cols + k_cols] = jnp.dot(normed, wk_ref[...], preferred_element_type=F32).astype(BF16)
        pj[c, :, q_cols + k_cols:cols] = jnp.dot(normed, wv_ref[...], preferred_element_type=F32).astype(BF16)
        s1(c).start()
        if c >= 1:
            mid(c - 1)
    mid(steps - 1)
    for c in range(steps):
        last(c)
    for c in range(steps):
        s3(c, give).wait_recv()
    for k in range(3):
        stat[k].wait_send()
    for c in range(steps):
        s1(c).wait_send()
        s2(c).wait_send()
        s3(c, keep).wait_send()


def front(x_in, gain, w_q, w_k, w_v, steps, width_full):
    rows, width = x_in.shape
    nb = rows // steps
    cols = w_q.shape[1] + 2 * w_k.shape[1]
    hb = nb // 2
    dma = pltpu.SemaphoreType.DMA
    vm = pl.BlockSpec(memory_space=pltpu.VMEM)
    return pl.pallas_call(
        functools.partial(front_body, width_full=width_full),
        out_shape=jax.ShapeDtypeStruct((steps, nb, cols), BF16),
        in_specs=[vm] * 5,
        out_specs=vm,
        scratch_shapes=[
            pltpu.VMEM((8, LANE), F32), pltpu.VMEM((3, 8, LANE), F32),
            pltpu.VMEM((rows, width), BF16), pltpu.VMEM((steps, nb, cols), BF16),
            pltpu.VMEM((steps, hb, cols), BF16), pltpu.VMEM((steps, hb, cols), BF16), pltpu.VMEM((steps, hb, cols), BF16),
            dma((3,)), dma((3,)), dma((steps,)), dma((steps,)), dma((steps,)), dma((steps,)), dma((steps,)), dma((steps,)),
        ],
        compiler_params=pltpu.CompilerParams(collective_id=2, has_side_effects=True, vmem_limit_bytes=60 * MIB),
        cost_estimate=pl.CostEstimate(flops=2 * rows * width * cols, bytes_accessed=4 * MIB, transcendentals=0),
    )(x_in, gain, w_q, w_k, w_v)


def tail_body(mix_ref, wo_ref, xin_ref, g_ref, wr_ref, ch_ref, wact_hbm, wlin_hbm, wdn_hbm, out_ref,
              wcat, wdn, pa, ar, xm, hh, st, st_in, hs, rs1, cs, rs2, lgp, lr1, lcs, lr2, u, pd, yr,
              wsem, as_, ar_s, xs, xr, sts, str_, s1s, s1r, s2s, s2r, l1s, l1r, l2s, l2r, us, ur, ys, yrs, gs, gr, *, width_full):
    experts = wcat.shape[0]
    ff = wact_hbm.shape[2]
    steps, top, nb = ch_ref.shape
    parts = rs1.shape[0]
    per = parts // steps
    ns = nb // per
    hb, qb = ns // 2, ns // 4
    dp, y, x = lax.axis_index("dp"), lax.axis_index("y"), lax.axis_index("x")
    core, chip = x % 2, x // 2
    sib = (dp, y, chip * 2 + (1 - core))
    peer = (dp, y, (1 - chip) * 2 + core)
    diag = (dp, y, (1 - chip) * 2 + (1 - core))
    near = (sib, peer, diag)
    hops = range(1, NEAR + 1)
    ypeer = [None] + [(dp, (y + d) % (NEAR + 1), x) for d in hops]
    slots = range(NEAR)
    nothing = (((1,), (1,)), ((), ()))

    w0 = pltpu.make_async_copy(wact_hbm, wcat.at[:, :, pl.ds(0, ff)], wsem.at[0])
    w1 = pltpu.make_async_copy(wlin_hbm, wcat.at[:, :, pl.ds(ff, ff)], wsem.at[1])
    w2 = pltpu.make_async_copy(wdn_hbm, wdn, wsem.at[2])
    barrier = pltpu.get_barrier_semaphore()
    for dev in near + tuple(ypeer[1:]):
        pl.semaphore_signal(barrier, inc=1, device_id=dev, device_id_type=MESH)

    def rows(k, start, size):
        return pl.ds(pl.multiple_of(k * ns + start, SUB), size)

    keep, give = core * hb, (1 - core) * hb
    sub_keep, sub_give = chip * qb, (1 - chip) * qb
    own, other = keep + sub_keep, keep + sub_give
    sib_own, sib_other = give + sub_keep, give + sub_give

    def ydist(d):
        return ((y + d) % (NEAR + 1)) * qb

    def rs_send(buf, land, ssem, rsem, k, d):
        return remote(buf.at[rows(k, ydist(d), qb), :], land.at[k, NEAR - d], ssem.at[k, d - 1], rsem.at[k, NEAR - d], ypeer[d])

    def rs_recv(buf, land, ssem, rsem, k, i):
        return remote(buf.at[rows(k, 0, qb), :], land.at[k, i], ssem.at[k, i], rsem.at[k, i], ypeer[1])

    def ag_send(buf, ssem, rsem, k, d):
        mine = buf.at[rows(k, y * qb, qb), :]
        return remote(mine, mine, ssem.at[k, d - 1], rsem.at[k, NEAR - d], ypeer[d])

    def ag_recv(buf, ssem, rsem, k, i):
        theirs = buf.at[rows(k, ydist(i + 1), qb), :]
        return remote(theirs, theirs, ssem.at[k, i], rsem.at[k, i], ypeer[1])

    def s1(k):
        return remote(hs.at[rows(k, give, hb), :], rs1.at[k], s1s.at[k], s1r.at[k], sib)

    def s2(k):
        return remote(cs.at[k], rs2.at[k], s2s.at[k], s2r.at[k], peer)

    def l1(k):
        return remote(lgp.at[rows(k, give, hb), :], lr1.at[k], l1s.at[k], l1r.at[k], sib)

    def l2(k):
        return remote(lcs.at[k], lr2.at[k], l2s.at[k], l2r.at[k], peer)

    def u_copy(k, row, i):
        blk = u.at[rows(k, row, qb), :]
        return remote(blk, blk, us.at[k, i], ur.at[k, i], peer if i == 0 else sib)

    def stat(k, i):
        return remote(st.at[k], st_in.at[k, i], sts.at[k, i], str_.at[k, i], near[i])

    def attn_out(c):
        pa[c * nb:(c + 1) * nb, :] = jnp.dot(mix_ref[c], wo_ref[...], preferred_element_type=F32).astype(BF16)

    def attn_send(k):
        for d in hops:
            rs_send(pa, ar, as_, ar_s, k, d).start()

    def attn_sum(k):
        for i in slots:
            rs_recv(pa, ar, as_, ar_s, k, i).wait_recv()
        acc = pa[rows(k, y * qb, qb), :].astype(F32)
        for i in slots:
            acc = acc + ar[k, i].astype(F32)
        mid = (xin_ref[rows(k, y * qb, qb), :].astype(F32) + acc).astype(BF16)
        xm[k] = mid
        st[k] = square_lanes(mid.astype(F32))
        for i in slots:
            stat(k, i).start()

    def norm(k):
        for i in slots:
            stat(k, i).wait_recv()
        total = st[k]
        for i in slots:
            total = total + st_in[k, i]
        scale = lax.rsqrt(jnp.sum(total, axis=1, keepdims=True) / width_full + EPS)
        hh[rows(k, y * qb, qb), :] = (xm[k].astype(F32) * scale * g_ref[1:2, :]).astype(BF16)
        for d in hops:
            ag_send(hh, xs, xr, k, d).start()

    def ready(c):
        for k in range(c * per, (c + 1) * per):
            for i in slots:
                ag_recv(hh, xs, xr, k, i).wait_recv()
        blk = slice(c * nb, (c + 1) * nb)
        lgp[blk, 0:experts] = lax.dot_general(hh[blk, :], wr_ref[...], nothing, preferred_element_type=F32)
        for k in range(c * per, (c + 1) * per):
            l1(k).start()

    def experts_in(c, part, hd):
        span = 4
        half = experts // span // 2

        def few(i, carry):
            for q in range(span):
                e = i * span + q
                hval = jnp.dot(hh[c * nb:(c + 1) * nb, :], wcat[e], preferred_element_type=F32)
                hd[e] = hval[:, 0:ff].astype(BF16)
                hd[experts + e] = hval[:, ff:2 * ff].astype(BF16)
            return carry
        lax.fori_loop(part * half, (part + 1) * half, few, 0)

    def pick(k, hd, chs):
        def tile(i, carry):
            r = pl.multiple_of((k % per) * ns + i * SUB, SUB)
            ch = [chs[j, rows(k, i * SUB, SUB), :] for j in range(top)]
            span = 8

            def some(g, state):
                acc, ev = list(state[0]), state[1]
                for q in range(span):
                    e = g * span + q
                    va = hd[e, pl.ds(r, SUB), :]
                    vl = hd[experts + e, pl.ds(r, SUB), :]
                    for j in range(top):
                        m = ch[j] == ev
                        acc[2 * j] = jnp.where(m, va, acc[2 * j])
                        acc[2 * j + 1] = jnp.where(m, vl, acc[2 * j + 1])
                    ev = ev + jnp.ones_like(ev)
                return tuple(acc), ev
            zero = jnp.zeros((SUB, ff), BF16)
            acc, _ = lax.fori_loop(0, experts // span, some, (tuple(zero for _ in range(2 * top)), zero))
            for q in range(2 * top):
                hs[rows(k, i * SUB, SUB), q * ff:(q + 1) * ff] = acc[q]
            return carry
        lax.fori_loop(0, ns // SUB, tile, 0)
        s1(k).start()

    def experts_pick(c, part, k, hd, prior, chs):
        rounds = 4
        span, tiles = experts // 2 // rounds, ns // SUB // rounds

        def both(i, carry):
            for q in range(span):
                e = part * (experts // 2) + i * span + q
                hval = jnp.dot(hh[c * nb:(c + 1) * nb, :], wcat[e], preferred_element_type=F32)
                hd[e] = hval[:, 0:ff].astype(BF16)
                hd[experts + e] = hval[:, ff:2 * ff].astype(BF16)
            for q in range(tiles):
                row = (i * tiles + q) * SUB
                r = pl.ds(pl.multiple_of((k % per) * ns + row, SUB), SUB)
                ch = [chs[j, rows(k, row, SUB), :] for j in range(top)]
                acc = [jnp.zeros((SUB, ff), BF16) for _ in range(2 * top)]
                for e in range(experts):
                    va, vl = prior[e, r, :], prior[experts + e, r, :]
                    for j in range(top):
                        m = ch[j] == jnp.asarray(e, BF16)
                        acc[2 * j] = jnp.where(m, va, acc[2 * j])
                        acc[2 * j + 1] = jnp.where(m, vl, acc[2 * j + 1])
                for j in range(2 * top):
                    hs[rows(k, row, SUB), j * ff:(j + 1) * ff] = acc[j]
            return carry
        lax.fori_loop(0, rounds, both, 0)
        s1(k).start()

    def logits_mid(k):
        l1(k).wait_recv()
        lcs[k] = lgp[rows(k, other, qb), :] + lr1[k, pl.ds(pl.multiple_of(sub_give, SUB), qb), :]
        l2(k).start()

    def part_b(k):
        logits_mid(k)
        s1(k).wait_recv()

        def add(i, carry):
            mine = hs[rows(k, other + i * SUB, SUB), :].astype(F32)
            got = rs1[k, pl.ds(pl.multiple_of(sub_give + i * SUB, SUB), SUB), :].astype(F32)
            cs[k, pl.ds(pl.multiple_of(i * SUB, SUB), SUB), :] = (mine + got).astype(BF16)
            return carry
        lax.fori_loop(0, qb // SUB, add, 0)
        s2(k).start()

    def part_u(k, chs):
        l2(k).wait_recv()
        s2(k).wait_recv()

        def tile(i, carry):
            r = pl.ds(pl.multiple_of(i * SUB, SUB), SUB)
            r_own = rows(k, own + i * SUB, SUB)
            r_sub = pl.ds(pl.multiple_of(sub_keep + i * SUB, SUB), SUB)
            logit = lgp[r_own, :] + lr1[k, r_sub, :] + lr2[k, r, :]
            lane = lax.broadcasted_iota(jnp.int32, (SUB, LANE), 1).astype(F32)
            hit = [chs[j, r_own, :].astype(F32) == lane for j in range(top)]
            any_hit = hit[0]
            for j in range(1, top):
                any_hit = any_hit | hit[j]
            peak = jnp.max(jnp.where(any_hit, logit, -jnp.inf), axis=1, keepdims=True)
            ex = jnp.where(any_hit, jnp.exp(logit - peak), 0.0)
            coef = ex / jnp.sum(ex, axis=1, keepdims=True)
            for j in range(top):
                gate = jnp.sum(jnp.where(hit[j], coef, 0.0), axis=1, keepdims=True)
                ca, cl = pl.ds(2 * j * ff, ff), pl.ds((2 * j + 1) * ff, ff)
                act = hs[r_own, ca].astype(F32) + rs1[k, r_sub, ca].astype(F32) + rs2[k, r, ca].astype(F32)
                lin = hs[r_own, cl].astype(F32) + rs1[k, r_sub, cl].astype(F32) + rs2[k, r, cl].astype(F32)
                val = gate * (act / (1.0 + jnp.exp(-act))) * lin
                u[r_own, j * ff:(j + 1) * ff] = val.astype(BF16)
            return carry
        lax.fori_loop(0, qb // SUB, tile, 0)
        u_copy(k, own, 0).start()
        u_copy(k, own, 1).start()

    def part_f(k):
        u_copy(k, other, 0).wait_recv()
        u_copy(k, other, 2).start()

    def part_d(k, ud, chs, us16):
        u_copy(k, sib_own, 1).wait_recv()
        u_copy(k, sib_other, 2).wait_recv()
        for j in range(top):
            us16[j] = u[k * ns:(k + 1) * ns, j * ff:(j + 1) * ff]

        def spread(i, carry):
            r = pl.ds(pl.multiple_of(i * SUB, SUB), SUB)
            ch = [chs[j, rows(k, i * SUB, SUB), :] for j in range(top)]
            vals = [us16[j, r, :] for j in range(top)]
            for e in range(experts):
                acc = jnp.zeros((SUB, ff), BF16)
                for j in range(top):
                    acc = jnp.where(ch[j] == jnp.asarray(e, BF16), vals[j], acc)
                ud[r, e * ff:(e + 1) * ff] = acc
            return carry
        lax.fori_loop(0, ns // SUB, spread, 0)
        pd[k * ns:(k + 1) * ns, :] = jnp.dot(ud[...], wdn[...], preferred_element_type=F32).astype(BF16)
        for d in hops:
            rs_send(pd, yr, ys, yrs, k, d).start()

    def part_g(k):
        for i in slots:
            rs_recv(pd, yr, ys, yrs, k, i).wait_recv()
        acc = pd[rows(k, y * qb, qb), :].astype(F32)
        for i in slots:
            acc = acc + yr[k, i].astype(F32)
        out_ref[rows(k, y * qb, qb), :] = (xm[k].astype(F32) + acc).astype(BF16)
        for d in hops:
            ag_send(out_ref, gs, gr, k, d).start()

    def run(hda, hdb, ud, chs, us16):
        w0.start()
        w1.start()
        w2.start()
        for c in range(steps):
            attn_out(c)
        lgp[...] = jnp.zeros_like(lgp)
        for c in range(steps):
            for i in range(nb // LANE):
                for j in range(top):
                    row = ch_ref[c, j:j + 1, LANE * i:LANE * (i + 1)].astype(F32)
                    chs[j, c * nb + LANE * i:c * nb + LANE * (i + 1), :] = jnp.broadcast_to(row, (LANE, LANE)).T.astype(BF16)
        pl.semaphore_wait(barrier, 2 * NEAR)
        attn_send(0)
        attn_send(1)
        attn_sum(0)
        attn_sum(1)
        norm(0)
        norm(1)
        attn_send(2)
        attn_send(3)
        ready(0)
        attn_send(4)
        attn_send(5)
        w0.wait()
        w1.wait()
        experts_in(0, 0, hda)
        attn_sum(2)
        attn_sum(3)
        experts_in(0, 1, hda)
        norm(2)
        norm(3)
        pick(0, hda, chs)
        attn_sum(4)
        attn_sum(5)
        pick(1, hda, chs)
        part_b(0)
        norm(4)
        norm(5)
        part_b(1)
        ready(1)
        experts_in(1, 0, hdb)
        experts_in(1, 1, hdb)
        part_u(0, chs)
        pick(2, hdb, chs)
        part_u(1, chs)
        part_b(2)
        ready(2)
        experts_pick(2, 0, 3, hda, hdb, chs)
        part_f(0)
        part_b(3)
        w2.wait()
        part_d(0, ud, chs, us16)
        part_u(2, chs)
        part_f(1)
        experts_in(2, 1, hda)
        pick(4, hda, chs)
        part_u(3, chs)
        part_g(0)
        part_d(1, ud, chs, us16)
        part_b(4)
        pick(5, hda, chs)
        part_f(2)
        part_b(5)
        part_d(2, ud, chs, us16)
        part_g(1)
        part_f(3)
        part_u(4, chs)
        part_d(3, ud, chs, us16)
        part_g(2)
        part_u(5, chs)
        part_f(4)
        part_d(4, ud, chs, us16)
        part_f(5)
        part_g(3)
        part_d(5, ud, chs, us16)
        part_g(4)
        part_g(5)

    bf = functools.partial(pltpu.VMEM, dtype=BF16)
    pl.run_scoped(run, bf((2 * experts, nb, ff)), bf((2 * experts, nb, ff)), bf((ns, experts * ff)), bf((top, steps * nb, ff)), bf((top, ns, ff)))

    for k in range(parts):
        for i in slots:
            ag_recv(out_ref, gs, gr, k, i).wait_recv()
    for k in range(parts):
        for i in slots:
            stat(k, i).wait_send()
        l1(k).wait_send()
        l2(k).wait_send()
        s1(k).wait_send()
        s2(k).wait_send()
        u_copy(k, own, 0).wait_send()
        u_copy(k, own, 1).wait_send()
        u_copy(k, other, 2).wait_send()
        for d in hops:
            rs_send(pa, ar, as_, ar_s, k, d).wait_send()
            ag_send(hh, xs, xr, k, d).wait_send()
            rs_send(pd, yr, ys, yrs, k, d).wait_send()
            ag_send(out_ref, gs, gr, k, d).wait_send()


def tail(mixed, wo, x_in, gain, w_router, chosen, w_act, w_lin, w_down, width_full):
    total, width = x_in.shape
    steps, top, nb = chosen.shape
    experts, _, ff = w_act.shape
    parts = 2 * steps
    ns = nb // 2
    hb, qb = ns // 2, ns // 4
    dma = pltpu.SemaphoreType.DMA
    vm = pl.BlockSpec(memory_space=pltpu.VMEM)
    hbm = pl.BlockSpec(memory_space=pl.ANY)
    bf = functools.partial(pltpu.VMEM, dtype=BF16)
    fl = functools.partial(pltpu.VMEM, dtype=F32)
    wide = 2 * top * ff
    each, three = (parts,), (parts, NEAR)
    sems = [three] * 6 + [each] * 8 + [three] * 6
    return pl.pallas_call(
        functools.partial(tail_body, width_full=width_full),
        out_shape=jax.ShapeDtypeStruct((total, width), BF16),
        in_specs=[vm] * 6 + [hbm] * 3,
        out_specs=vm,
        scratch_shapes=[
            bf((experts, width, 2 * ff)), bf((experts * ff, width)),
            bf((total, width)), bf((parts, NEAR, qb, width)), bf((parts, qb, width)), bf((total, width)),
            fl((parts, qb, LANE)), fl((parts, NEAR, qb, LANE)),
            bf((total, wide)), bf((parts, hb, wide)), bf((parts, qb, wide)), bf((parts, qb, wide)),
            fl((total, LANE)), fl((parts, hb, LANE)), fl((parts, qb, LANE)), fl((parts, qb, LANE)),
            bf((total, top * ff)), bf((total, width)), bf((parts, NEAR, qb, width)),
            dma((NEAR,)),
        ] + [dma(n) for n in sems],
        compiler_params=pltpu.CompilerParams(collective_id=1, has_side_effects=True, vmem_limit_bytes=60 * MIB),
        cost_estimate=pl.CostEstimate(flops=6 * total * width * experts * ff, bytes_accessed=12 * MIB, transcendentals=0),
    )(mixed, wo, x_in, gain, w_router, chosen, w_act, w_lin, w_down.reshape(experts * ff, width))


def solution(mesh):
    x_count = mesh.shape['x']
    cache_spec = P('dp', None, 'y', None)
    in_specs = (P(None, 'dp'), P('dp'), P(None, 'dp', None), P(None, 'x'), cache_spec, cache_spec, P('x'), P('x', 'y'), P('x', 'y'), P('x', 'y'), P('y', 'x'), P('x'), P('x', None), P(None, 'x', 'y'), P(None, 'x', 'y'), P(None, 'y', 'x'))
    out_specs = (P(None, 'dp', 'x'), cache_spec, cache_spec)

    def per_device(tokens, lengths, choices, emb_table, k_cache, v_cache, g_attn, w_q, w_k, w_v, w_o, g_ffn, w_router, w_act, w_lin, w_down):
        steps, nb = tokens.shape
        seq, kvl, hdim = k_cache.shape[1:]
        q_cols, kv_cols = w_q.shape[1], w_k.shape[1]
        width = emb_table.shape[1]
        width_full = width * x_count
        group = q_cols // kv_cols
        rows = steps * nb
        x_in = emb_table.at[tokens].get(mode="promise_in_bounds").reshape(rows, width)
        line = lax.broadcasted_iota(jnp.int32, (3, width), 0)
        spread = jnp.pad(lengths.astype(F32), (0, width - nb))
        gains = jnp.where(line == 0, g_attn.astype(F32)[None, :], jnp.where(line == 1, g_ffn.astype(F32)[None, :], spread[None, :]))
        proj = front(x_in, gains, w_q, w_k, w_v, steps, width_full)
        kc = k_cache.transpose(0, 2, 3, 1).reshape(nb, kv_cols, seq)
        vc = v_cache.transpose(0, 2, 3, 1).reshape(nb, kv_cols, seq)
        mixed, ko, vo = attention(lengths, proj, kc, vc, group)
        hidden = tail(mixed, w_o, x_in, gains, w_router.T, choices.transpose(0, 2, 1), w_act, w_lin, w_down, width_full).reshape(steps, nb, width)
        ko = ko.reshape(nb, kvl, hdim, seq).transpose(0, 3, 1, 2)
        vo = vo.reshape(nb, kvl, hdim, seq).transpose(0, 3, 1, 2)
        return hidden, ko, vo

    return jax.shard_map(per_device, mesh=mesh, in_specs=in_specs, out_specs=out_specs, check_vma=False)
```

```python
import functools
import jax
import jax.numpy as jnp
from jax import lax
from jax.experimental import pallas as pl
from jax.experimental.pallas import tpu as pltpu
from jax.sharding import PartitionSpec as P

EPS = 1e-5
ROPE_BASE = 1.0e6
MESH = pl.DeviceIdType.MESH
F32 = jnp.float32
BF16 = jnp.bfloat16
LANE = 128
SUB = 16
MIB = 1024 * 1024
LOWEST = -1.0e30
NB = 32
QROWS = 16
HEAD = 64
NEAR = 3


def attn_body(len_ref, q_ref, kn_ref, vn_ref, k_ref, v_ref, o_ref, ko_ref, vo_ref, s_ref, w_ref, qs, ks, vs, os_, *, group):
    half, seq = k_ref.shape[1:]
    steps, n_seq = q_ref.shape[:2]
    step = pl.program_id(0)

    @pl.when(step == 0)
    def _():
        for ref in (qs, ks, vs):
            ref[...] = jnp.zeros_like(ref)

    for t in range(steps):
        ks[pl.ds(t, n_seq, stride=steps), :] = kn_ref[t].astype(F32)
        vs[pl.ds(t, n_seq, stride=steps), :] = vn_ref[t].astype(F32)
        for g in range(group):
            qs[pl.ds(t * group + g, n_seq, stride=QROWS), :] = q_ref[t, :, LANE * g:LANE * (g + 1)].astype(F32)
    kn_t = ks[...].T
    vn_t = vs[...].T
    lane = lax.broadcasted_iota(jnp.int32, (SUB, LANE), 1).astype(F32).astype(BF16)
    srow = lax.broadcasted_iota(jnp.int32, (2 * QROWS, seq), 0)
    scol = lax.broadcasted_iota(jnp.int32, (2 * QROWS, seq), 1)
    srow = jnp.where(srow >= QROWS, srow - QROWS, srow)
    rel = scol - jnp.where(srow >= 2 * group, 2, jnp.where(srow >= group, 1, 0))
    low = lax.broadcasted_iota(jnp.int32, (QROWS, LANE), 1) < HEAD
    low_b = lane < jnp.asarray(HEAD, BF16)
    for b in range(n_seq):
        pos = len_ref[step * n_seq + b]
        turn = lax.rem(pos + LANE - b * steps, LANE)
        new = (pltpu.roll(kn_t, turn, 1).astype(BF16), pltpu.roll(vn_t, turn, 1).astype(BF16))
        gap = lane - jnp.full((SUB, LANE), pos.astype(F32), F32).astype(BF16)
        for tile in range(seq // LANE):
            lo = jnp.asarray(-LANE * tile, BF16)
            hi = jnp.asarray(steps - 1 - LANE * tile, BF16)
            hit = (gap >= lo) & (gap <= hi)
            for i in range(half // SUB):
                rs, cs = slice(SUB * i, SUB * i + SUB), slice(LANE * tile, LANE * tile + LANE)
                ko_ref[b, rs, cs] = jnp.where(hit, new[0][rs], k_ref[b, rs, cs])
                vo_ref[b, rs, cs] = jnp.where(hit, new[1][rs], v_ref[b, rs, cs])
    for b in range(n_seq):
        q16 = qs[QROWS * b:QROWS * (b + 1), :].astype(BF16)
        zero = jnp.zeros_like(q16)
        q32 = jnp.concatenate([jnp.where(low_b, q16, zero), jnp.where(low_b, zero, q16)], axis=0)
        s_ref[b] = jnp.dot(q32, ko_ref[b], preferred_element_type=F32)
    tots = []
    for b in range(n_seq):
        pos = len_ref[step * n_seq + b]
        ok = rel <= pos
        s = jnp.where(ok, s_ref[b] * HEAD ** -0.5, LOWEST)
        peak = jnp.max(s, axis=1, keepdims=True)
        w = jnp.where(ok, jnp.exp(s - peak), 0.0)
        tots.append(jnp.sum(w, axis=1, keepdims=True))
        w_ref[b] = w.astype(BF16)
    for b in range(n_seq):
        o = lax.dot_general(w_ref[b], vo_ref[b], (((1,), (1,)), ((), ())), preferred_element_type=F32)
        o = o / tots[b]
        os_[QROWS * b:QROWS * (b + 1), :] = jnp.where(low, o[:QROWS], o[QROWS:])
    for t in range(steps):
        og = [os_[pl.ds(t * group + g, n_seq, stride=QROWS), :] for g in range(group)]
        turned = pltpu.roll(og[1], HEAD, 1)
        first = lax.broadcasted_iota(jnp.int32, (n_seq, LANE), 1) < HEAD
        tiles = (jnp.where(first, og[0], turned), jnp.where(first, og[2], og[0]), jnp.where(first, turned, og[2]))
        for g in range(group):
            o_ref[t, :, LANE * g:LANE * (g + 1)] = tiles[g].astype(BF16)


def attention(lengths, proj, kc, vc, group):
    nb, half, seq = kc.shape
    steps = proj.shape[0]
    cache = pl.BlockSpec((NB, half, seq), lambda i, l: (i, 0, 0))
    qs = pl.BlockSpec((steps, NB, group * LANE), lambda i, l: (0, i, 0))
    kspec = pl.BlockSpec((steps, NB, LANE), lambda i, l: (0, i, group))
    vspec = pl.BlockSpec((steps, NB, LANE), lambda i, l: (0, i, group + 1))
    flat = pltpu.VMEM((NB * QROWS, LANE), F32)
    new = pltpu.VMEM((LANE, LANE), F32)
    return pl.pallas_call(
        functools.partial(attn_body, group=group),
        grid_spec=pltpu.PrefetchScalarGridSpec(num_scalar_prefetch=1, grid=(nb // NB,), in_specs=[qs, kspec, vspec, cache, cache], out_specs=[qs, cache, cache],
            scratch_shapes=[pltpu.VMEM((NB, 2 * QROWS, seq), F32), pltpu.VMEM((NB, 2 * QROWS, seq), BF16), flat, new, new, flat]),
        out_shape=[jax.ShapeDtypeStruct((steps, nb, group * LANE), BF16), jax.ShapeDtypeStruct(kc.shape, BF16), jax.ShapeDtypeStruct(vc.shape, BF16)],
        compiler_params=pltpu.CompilerParams(vmem_limit_bytes=60 * MIB, dimension_semantics=("arbitrary",)),
        cost_estimate=pl.CostEstimate(flops=2 * nb * 32 * LANE * seq * 2, bytes_accessed=4 * nb * half * seq * 2, transcendentals=0),
    )(lengths, proj, proj, proj, kc, vc)


def remote(src, dst, ssem, rsem, dev):
    return pltpu.make_async_remote_copy(src_ref=src, dst_ref=dst, send_sem=ssem, recv_sem=rsem, device_id=dev, device_id_type=MESH)


def square_lanes(x_f32):
    acc = x_f32[:, 0:LANE] * x_f32[:, 0:LANE]
    for i in range(1, x_f32.shape[1] // LANE):
        part = x_f32[:, LANE * i:LANE * (i + 1)]
        acc = acc + part * part
    return acc


def square_rows(x_f32):
    return jnp.sum(square_lanes(x_f32).T, axis=0, keepdims=True)


def scale_rows(x_f32, stat_row, gain, width_full):
    scale = lax.rsqrt(stat_row / width_full + EPS)
    col = jnp.broadcast_to(scale, (LANE, LANE)).T
    parts = [x_f32[:, LANE * i:LANE * (i + 1)] * col * gain[:, LANE * i:LANE * (i + 1)] for i in range(x_f32.shape[1] // LANE)]
    return jnp.concatenate(parts, axis=1).astype(BF16)


def front_body(x_ref, g_ref, wq_ref, wk_ref, wv_ref, out_ref, st, st_in, hh, pj, rs1, cs, rs2, sts, str_, s1s, s1r, s2s, s2r, s3s, s3r, *, width_full):
    steps, nb = out_ref.shape[:2]
    q_cols, k_cols = wq_ref.shape[1], wk_ref.shape[1]
    gain = g_ref[0:1, :]
    cols = out_ref.shape[2]
    hb = nb // 2
    dp, y, x = lax.axis_index("dp"), lax.axis_index("y"), lax.axis_index("x")
    core, chip = x % 2, x // 2
    sib = (dp, y, chip * 2 + (1 - core))
    peer = (dp, y, (1 - chip) * 2 + core)
    diag = (dp, y, (1 - chip) * 2 + (1 - core))
    near = (sib, peer, diag)
    barrier = pltpu.get_barrier_semaphore()
    for dev in near:
        pl.semaphore_signal(barrier, inc=1, device_id=dev, device_id_type=MESH)
    keep = pl.multiple_of(core * hb, hb)
    give = pl.multiple_of((1 - core) * hb, hb)
    st[...] = jnp.zeros_like(st)
    blocks = steps * nb // LANE
    for i in range(blocks):
        st[i:i + 1, :] = square_rows(x_ref[LANE * i:LANE * (i + 1), :].astype(F32))
    pl.semaphore_wait(barrier, 3)
    stat = [remote(st, st_in.at[k], sts.at[k], str_.at[k], near[k]) for k in range(3)]
    for k in range(3):
        stat[k].start()
    for k in range(3):
        stat[k].wait_recv()
    total = st[...] + st_in[0] + st_in[1] + st_in[2]

    def s1(c):
        return remote(pj.at[c, pl.ds(give, hb), :], rs1.at[c], s1s.at[c], s1r.at[c], sib)

    def s2(c):
        return remote(cs.at[c], rs2.at[c], s2s.at[c], s2r.at[c], peer)

    def s3(c, row):
        return remote(out_ref.at[c, pl.ds(row, hb), :], out_ref.at[c, pl.ds(row, hb), :], s3s.at[c], s3r.at[c], sib)

    def mid(c):
        s1(c).wait_recv()
        cs[c] = (pj[c, pl.ds(keep, hb), :].astype(F32) + rs1[c].astype(F32)).astype(BF16)
        s2(c).start()

    def last(c):
        lane = lax.broadcasted_iota(jnp.int32, (hb, LANE), 1)
        inv_freq = ROPE_BASE ** (-((lane % (HEAD // 2)).astype(F32) * 2.0 / HEAD))
        length = jnp.broadcast_to(g_ref[2:3, pl.ds(keep, hb)], (LANE, hb)).T
        angle = (length + float(c)) * inv_freq
        first, low = lane % HEAD < HEAD // 2, lane < HEAD
        cosv, sinv = jnp.cos(angle), jnp.sin(angle)
        sinv = jnp.where(first, -sinv, sinv)
        s2(c).wait_recv()
        fin = (cs[c].astype(F32) + rs2[c].astype(F32)).astype(BF16).astype(F32)
        tiles = [fin[:, LANE * i:LANE * (i + 1)] for i in range(cols // LANE)]
        for i in range((q_cols + k_cols) // LANE):
            v = tiles[i]
            swap = jnp.where(first, pltpu.roll(v, LANE - HEAD // 2, 1), pltpu.roll(v, HEAD // 2, 1))
            tiles[i] = v * cosv + swap * sinv
        ta, tb, tc = tiles[:NEAR]
        tiles[:NEAR] = [jnp.where(low, ta, tb), pltpu.roll(jnp.where(low, tc, ta), HEAD, 1), jnp.where(low, tb, tc)]
        for i in range(cols // LANE):
            out_ref[c, pl.ds(keep, hb), LANE * i:LANE * (i + 1)] = tiles[i].astype(BF16)
        s3(c, keep).start()

    for c in range(steps):
        for i in range(c * nb // LANE, (c + 1) * nb // LANE):
            hh[LANE * i:LANE * (i + 1), :] = scale_rows(x_ref[LANE * i:LANE * (i + 1), :].astype(F32), total[i:i + 1, :], gain, width_full)
        normed = hh[c * nb:(c + 1) * nb, :]
        pj[c, :, 0:q_cols] = jnp.dot(normed, wq_ref[...], preferred_element_type=F32).astype(BF16)
        pj[c, :, q_cols:q_cols + k_cols] = jnp.dot(normed, wk_ref[...], preferred_element_type=F32).astype(BF16)
        pj[c, :, q_cols + k_cols:cols] = jnp.dot(normed, wv_ref[...], preferred_element_type=F32).astype(BF16)
        s1(c).start()
        if c >= 1:
            mid(c - 1)
    mid(steps - 1)
    for c in range(steps):
        last(c)
    for c in range(steps):
        s3(c, give).wait_recv()
    for k in range(3):
        stat[k].wait_send()
    for c in range(steps):
        s1(c).wait_send()
        s2(c).wait_send()
        s3(c, keep).wait_send()


def front(x_in, gain, w_q, w_k, w_v, steps, width_full):
    rows, width = x_in.shape
    nb = rows // steps
    cols = w_q.shape[1] + 2 * w_k.shape[1]
    hb = nb // 2
    dma = pltpu.SemaphoreType.DMA
    vm = pl.BlockSpec(memory_space=pltpu.VMEM)
    return pl.pallas_call(
        functools.partial(front_body, width_full=width_full),
        out_shape=jax.ShapeDtypeStruct((steps, nb, cols), BF16),
        in_specs=[vm] * 5,
        out_specs=vm,
        scratch_shapes=[
            pltpu.VMEM((8, LANE), F32), pltpu.VMEM((3, 8, LANE), F32),
            pltpu.VMEM((rows, width), BF16), pltpu.VMEM((steps, nb, cols), BF16),
            pltpu.VMEM((steps, hb, cols), BF16), pltpu.VMEM((steps, hb, cols), BF16), pltpu.VMEM((steps, hb, cols), BF16),
            dma((3,)), dma((3,)), dma((steps,)), dma((steps,)), dma((steps,)), dma((steps,)), dma((steps,)), dma((steps,)),
        ],
        compiler_params=pltpu.CompilerParams(collective_id=2, has_side_effects=True, vmem_limit_bytes=60 * MIB),
        cost_estimate=pl.CostEstimate(flops=2 * rows * width * cols, bytes_accessed=4 * MIB, transcendentals=0),
    )(x_in, gain, w_q, w_k, w_v)


def tail_body(mix_ref, wo_ref, xin_ref, g_ref, wr_ref, ch_ref, wact_hbm, wlin_hbm, wdn_hbm, out_ref,
              wcat, wdn, pa, ar, xm, hh, st, st_in, hs, rs1, cs, rs2, lgp, lr1, lcs, lr2, u, pd, yr,
              wsem, as_, ar_s, xs, xr, sts, str_, s1s, s1r, s2s, s2r, l1s, l1r, l2s, l2r, us, ur, ys, yrs, gs, gr, *, width_full):
    experts = wcat.shape[0]
    ff = wact_hbm.shape[2]
    steps, top, nb = ch_ref.shape
    parts = rs1.shape[0]
    per = parts // steps
    ns = nb // per
    hb, qb = ns // 2, ns // 4
    dp, y, x = lax.axis_index("dp"), lax.axis_index("y"), lax.axis_index("x")
    core, chip = x % 2, x // 2
    sib = (dp, y, chip * 2 + (1 - core))
    peer = (dp, y, (1 - chip) * 2 + core)
    diag = (dp, y, (1 - chip) * 2 + (1 - core))
    near = (sib, peer, diag)
    hops = range(1, NEAR + 1)
    ypeer = [None] + [(dp, (y + d) % (NEAR + 1), x) for d in hops]
    slots = range(NEAR)
    nothing = (((1,), (1,)), ((), ()))

    w0 = pltpu.make_async_copy(wact_hbm, wcat.at[:, :, pl.ds(0, ff)], wsem.at[0])
    w1 = pltpu.make_async_copy(wlin_hbm, wcat.at[:, :, pl.ds(ff, ff)], wsem.at[1])
    w2 = pltpu.make_async_copy(wdn_hbm, wdn, wsem.at[2])
    barrier = pltpu.get_barrier_semaphore()
    for dev in near + tuple(ypeer[1:]):
        pl.semaphore_signal(barrier, inc=1, device_id=dev, device_id_type=MESH)

    def rows(k, start, size):
        return pl.ds(pl.multiple_of(k * ns + start, SUB), size)

    keep, give = core * hb, (1 - core) * hb
    sub_keep, sub_give = chip * qb, (1 - chip) * qb
    own, other = keep + sub_keep, keep + sub_give
    sib_own, sib_other = give + sub_keep, give + sub_give

    def ydist(d):
        return ((y + d) % (NEAR + 1)) * qb

    def rs_send(buf, land, ssem, rsem, k, d):
        return remote(buf.at[rows(k, ydist(d), qb), :], land.at[k, NEAR - d], ssem.at[k, d - 1], rsem.at[k, NEAR - d], ypeer[d])

    def rs_recv(buf, land, ssem, rsem, k, i):
        return remote(buf.at[rows(k, 0, qb), :], land.at[k, i], ssem.at[k, i], rsem.at[k, i], ypeer[1])

    def ag_send(buf, ssem, rsem, k, d):
        mine = buf.at[rows(k, y * qb, qb), :]
        return remote(mine, mine, ssem.at[k, d - 1], rsem.at[k, NEAR - d], ypeer[d])

    def ag_recv(buf, ssem, rsem, k, i):
        theirs = buf.at[rows(k, ydist(i + 1), qb), :]
        return remote(theirs, theirs, ssem.at[k, i], rsem.at[k, i], ypeer[1])

    def s1(k):
        return remote(hs.at[rows(k, give, hb), :], rs1.at[k], s1s.at[k], s1r.at[k], sib)

    def s2(k):
        return remote(cs.at[k], rs2.at[k], s2s.at[k], s2r.at[k], peer)

    def l1(k):
        return remote(lgp.at[rows(k, give, hb), :], lr1.at[k], l1s.at[k], l1r.at[k], sib)

    def l2(k):
        return remote(lcs.at[k], lr2.at[k], l2s.at[k], l2r.at[k], peer)

    def u_copy(k, row, i):
        blk = u.at[rows(k, row, qb), :]
        return remote(blk, blk, us.at[k, i], ur.at[k, i], peer if i == 0 else sib)

    def stat(k, i):
        return remote(st.at[k], st_in.at[k, i], sts.at[k, i], str_.at[k, i], near[i])

    def attn_out(c):
        pa[c * nb:(c + 1) * nb, :] = jnp.dot(mix_ref[c], wo_ref[...], preferred_element_type=F32).astype(BF16)

    def attn_send(k):
        for d in hops:
            rs_send(pa, ar, as_, ar_s, k, d).start()

    def attn_sum(k):
        for i in slots:
            rs_recv(pa, ar, as_, ar_s, k, i).wait_recv()
        acc = pa[rows(k, y * qb, qb), :].astype(F32)
        for i in slots:
            acc = acc + ar[k, i].astype(F32)
        mid = (xin_ref[rows(k, y * qb, qb), :].astype(F32) + acc).astype(BF16)
        xm[k] = mid
        st[k] = square_lanes(mid.astype(F32))
        for i in slots:
            stat(k, i).start()

    def norm(k):
        for i in slots:
            stat(k, i).wait_recv()
        total = st[k]
        for i in slots:
            total = total + st_in[k, i]
        scale = lax.rsqrt(jnp.sum(total, axis=1, keepdims=True) / width_full + EPS)
        hh[rows(k, y * qb, qb), :] = (xm[k].astype(F32) * scale * g_ref[1:2, :]).astype(BF16)
        for d in hops:
            ag_send(hh, xs, xr, k, d).start()

    def ready(c):
        for k in range(c * per, (c + 1) * per):
            for i in slots:
                ag_recv(hh, xs, xr, k, i).wait_recv()
        blk = slice(c * nb, (c + 1) * nb)
        lgp[blk, 0:experts] = lax.dot_general(hh[blk, :], wr_ref[...], nothing, preferred_element_type=F32)
        for k in range(c * per, (c + 1) * per):
            l1(k).start()

    def experts_in(c, part, hd):
        span = 4
        half = experts // span // 2

        def few(i, carry):
            for q in range(span):
                e = i * span + q
                hval = jnp.dot(hh[c * nb:(c + 1) * nb, :], wcat[e], preferred_element_type=F32)
                hd[e] = hval[:, 0:ff].astype(BF16)
                hd[experts + e] = hval[:, ff:2 * ff].astype(BF16)
            return carry
        lax.fori_loop(part * half, (part + 1) * half, few, 0)

    def pick(k, hd, chs):
        def tile(i, carry):
            r = pl.multiple_of((k % per) * ns + i * SUB, SUB)
            ch = [chs[j, rows(k, i * SUB, SUB), :] for j in range(top)]
            span = 8

            def some(g, state):
                acc, ev = list(state[0]), state[1]
                for q in range(span):
                    e = g * span + q
                    va = hd[e, pl.ds(r, SUB), :]
                    vl = hd[experts + e, pl.ds(r, SUB), :]
                    for j in range(top):
                        m = ch[j] == ev
                        acc[2 * j] = jnp.where(m, va, acc[2 * j])
                        acc[2 * j + 1] = jnp.where(m, vl, acc[2 * j + 1])
                    ev = ev + jnp.ones_like(ev)
                return tuple(acc), ev
            zero = jnp.zeros((SUB, ff), BF16)
            acc, _ = lax.fori_loop(0, experts // span, some, (tuple(zero for _ in range(2 * top)), zero))
            for q in range(2 * top):
                hs[rows(k, i * SUB, SUB), q * ff:(q + 1) * ff] = acc[q]
            return carry
        lax.fori_loop(0, ns // SUB, tile, 0)
        s1(k).start()

    def experts_pick(c, part, k, hd, prior, chs):
        rounds = 4
        span, tiles = experts // 2 // rounds, ns // SUB // rounds

        def both(i, carry):
            for q in range(span):
                e = part * (experts // 2) + i * span + q
                hval = jnp.dot(hh[c * nb:(c + 1) * nb, :], wcat[e], preferred_element_type=F32)
                hd[e] = hval[:, 0:ff].astype(BF16)
                hd[experts + e] = hval[:, ff:2 * ff].astype(BF16)
            for q in range(tiles):
                row = (i * tiles + q) * SUB
                r = pl.ds(pl.multiple_of((k % per) * ns + row, SUB), SUB)
                ch = [chs[j, rows(k, row, SUB), :] for j in range(top)]
                acc = [jnp.zeros((SUB, ff), BF16) for _ in range(2 * top)]
                for e in range(experts):
                    va, vl = prior[e, r, :], prior[experts + e, r, :]
                    for j in range(top):
                        m = ch[j] == jnp.asarray(e, BF16)
                        acc[2 * j] = jnp.where(m, va, acc[2 * j])
                        acc[2 * j + 1] = jnp.where(m, vl, acc[2 * j + 1])
                for j in range(2 * top):
                    hs[rows(k, row, SUB), j * ff:(j + 1) * ff] = acc[j]
            return carry
        lax.fori_loop(0, rounds, both, 0)
        s1(k).start()

    def logits_mid(k):
        l1(k).wait_recv()
        lcs[k] = lgp[rows(k, other, qb), :] + lr1[k, pl.ds(pl.multiple_of(sub_give, SUB), qb), :]
        l2(k).start()

    def part_b(k):
        logits_mid(k)
        s1(k).wait_recv()

        def add(i, carry):
            mine = hs[rows(k, other + i * SUB, SUB), :].astype(F32)
            got = rs1[k, pl.ds(pl.multiple_of(sub_give + i * SUB, SUB), SUB), :].astype(F32)
            cs[k, pl.ds(pl.multiple_of(i * SUB, SUB), SUB), :] = (mine + got).astype(BF16)
            return carry
        lax.fori_loop(0, qb // SUB, add, 0)
        s2(k).start()

    def part_u(k, chs):
        l2(k).wait_recv()
        s2(k).wait_recv()

        def tile(i, carry):
            r = pl.ds(pl.multiple_of(i * SUB, SUB), SUB)
            r_own = rows(k, own + i * SUB, SUB)
            r_sub = pl.ds(pl.multiple_of(sub_keep + i * SUB, SUB), SUB)
            logit = lgp[r_own, :] + lr1[k, r_sub, :] + lr2[k, r, :]
            lane = lax.broadcasted_iota(jnp.int32, (SUB, LANE), 1).astype(F32)
            hit = [chs[j, r_own, :].astype(F32) == lane for j in range(top)]
            any_hit = hit[0]
            for j in range(1, top):
                any_hit = any_hit | hit[j]
            peak = jnp.max(jnp.where(any_hit, logit, -jnp.inf), axis=1, keepdims=True)
            ex = jnp.where(any_hit, jnp.exp(logit - peak), 0.0)
            coef = ex / jnp.sum(ex, axis=1, keepdims=True)
            for j in range(top):
                gate = jnp.sum(jnp.where(hit[j], coef, 0.0), axis=1, keepdims=True)
                ca, cl = pl.ds(2 * j * ff, ff), pl.ds((2 * j + 1) * ff, ff)
                act = hs[r_own, ca].astype(F32) + rs1[k, r_sub, ca].astype(F32) + rs2[k, r, ca].astype(F32)
                lin = hs[r_own, cl].astype(F32) + rs1[k, r_sub, cl].astype(F32) + rs2[k, r, cl].astype(F32)
                val = gate * (act / (1.0 + jnp.exp(-act))) * lin
                u[r_own, j * ff:(j + 1) * ff] = val.astype(BF16)
            return carry
        lax.fori_loop(0, qb // SUB, tile, 0)
        u_copy(k, own, 0).start()
        u_copy(k, own, 1).start()

    def part_f(k):
        u_copy(k, other, 0).wait_recv()
        u_copy(k, other, 2).start()

    def part_d(k, ud, chs, us16):
        u_copy(k, sib_own, 1).wait_recv()
        u_copy(k, sib_other, 2).wait_recv()
        for j in range(top):
            us16[j] = u[k * ns:(k + 1) * ns, j * ff:(j + 1) * ff]

        def spread(i, carry):
            r = pl.ds(pl.multiple_of(i * SUB, SUB), SUB)
            ch = [chs[j, rows(k, i * SUB, SUB), :] for j in range(top)]
            vals = [us16[j, r, :] for j in range(top)]
            for e in range(experts):
                acc = jnp.zeros((SUB, ff), BF16)
                for j in range(top):
                    acc = jnp.where(ch[j] == jnp.asarray(e, BF16), vals[j], acc)
                ud[r, e * ff:(e + 1) * ff] = acc
            return carry
        lax.fori_loop(0, ns // SUB, spread, 0)
        pd[k * ns:(k + 1) * ns, :] = jnp.dot(ud[...], wdn[...], preferred_element_type=F32).astype(BF16)
        for d in hops:
            rs_send(pd, yr, ys, yrs, k, d).start()

    def part_g(k):
        for i in slots:
            rs_recv(pd, yr, ys, yrs, k, i).wait_recv()
        acc = pd[rows(k, y * qb, qb), :].astype(F32)
        for i in slots:
            acc = acc + yr[k, i].astype(F32)
        out_ref[rows(k, y * qb, qb), :] = (xm[k].astype(F32) + acc).astype(BF16)
        for d in hops:
            ag_send(out_ref, gs, gr, k, d).start()

    def run(hda, hdb, ud, chs, us16):
        w0.start()
        w1.start()
        w2.start()
        for c in range(steps):
            attn_out(c)
        lgp[...] = jnp.zeros_like(lgp)
        for c in range(steps):
            for i in range(nb // LANE):
                for j in range(top):
                    row = ch_ref[c, j:j + 1, LANE * i:LANE * (i + 1)].astype(F32)
                    chs[j, c * nb + LANE * i:c * nb + LANE * (i + 1), :] = jnp.broadcast_to(row, (LANE, LANE)).T.astype(BF16)
        pl.semaphore_wait(barrier, 2 * NEAR)
        attn_send(0)
        attn_send(1)
        attn_sum(0)
        attn_sum(1)
        norm(0)
        norm(1)
        attn_send(2)
        attn_send(3)
        ready(0)
        attn_send(4)
        attn_send(5)
        w0.wait()
        w1.wait()
        experts_in(0, 0, hda)
        attn_sum(2)
        attn_sum(3)
        experts_in(0, 1, hda)
        norm(2)
        norm(3)
        pick(0, hda, chs)
        attn_sum(4)
        attn_sum(5)
        pick(1, hda, chs)
        part_b(0)
        norm(4)
        norm(5)
        part_b(1)
        ready(1)
        experts_in(1, 0, hdb)
        experts_in(1, 1, hdb)
        part_u(0, chs)
        pick(2, hdb, chs)
        part_u(1, chs)
        part_b(2)
        ready(2)
        experts_pick(2, 0, 3, hda, hdb, chs)
        part_f(0)
        w2.wait()
        part_d(0, ud, chs, us16)
        part_b(3)
        part_u(2, chs)
        part_f(1)
        experts_in(2, 1, hda)
        pick(4, hda, chs)
        part_u(3, chs)
        part_g(0)
        part_d(1, ud, chs, us16)
        part_b(4)
        pick(5, hda, chs)
        part_f(2)
        part_b(5)
        part_d(2, ud, chs, us16)
        part_g(1)
        part_f(3)
        part_u(4, chs)
        part_d(3, ud, chs, us16)
        part_g(2)
        part_u(5, chs)
        part_f(4)
        part_d(4, ud, chs, us16)
        part_f(5)
        part_g(3)
        part_d(5, ud, chs, us16)
        part_g(4)
        part_g(5)

    bf = functools.partial(pltpu.VMEM, dtype=BF16)
    pl.run_scoped(run, bf((2 * experts, nb, ff)), bf((2 * experts, nb, ff)), bf((ns, experts * ff)), bf((top, steps * nb, ff)), bf((top, ns, ff)))

    for k in range(parts):
        for i in slots:
            ag_recv(out_ref, gs, gr, k, i).wait_recv()
    for k in range(parts):
        for i in slots:
            stat(k, i).wait_send()
        l1(k).wait_send()
        l2(k).wait_send()
        s1(k).wait_send()
        s2(k).wait_send()
        u_copy(k, own, 0).wait_send()
        u_copy(k, own, 1).wait_send()
        u_copy(k, other, 2).wait_send()
        for d in hops:
            rs_send(pa, ar, as_, ar_s, k, d).wait_send()
            ag_send(hh, xs, xr, k, d).wait_send()
            rs_send(pd, yr, ys, yrs, k, d).wait_send()
            ag_send(out_ref, gs, gr, k, d).wait_send()


def tail(mixed, wo, x_in, gain, w_router, chosen, w_act, w_lin, w_down, width_full):
    total, width = x_in.shape
    steps, top, nb = chosen.shape
    experts, _, ff = w_act.shape
    parts = 2 * steps
    ns = nb // 2
    hb, qb = ns // 2, ns // 4
    dma = pltpu.SemaphoreType.DMA
    vm = pl.BlockSpec(memory_space=pltpu.VMEM)
    hbm = pl.BlockSpec(memory_space=pl.ANY)
    bf = functools.partial(pltpu.VMEM, dtype=BF16)
    fl = functools.partial(pltpu.VMEM, dtype=F32)
    wide = 2 * top * ff
    each, three = (parts,), (parts, NEAR)
    sems = [three] * 6 + [each] * 8 + [three] * 6
    return pl.pallas_call(
        functools.partial(tail_body, width_full=width_full),
        out_shape=jax.ShapeDtypeStruct((total, width), BF16),
        in_specs=[vm] * 6 + [hbm] * 3,
        out_specs=vm,
        scratch_shapes=[
            bf((experts, width, 2 * ff)), bf((experts * ff, width)),
            bf((total, width)), bf((parts, NEAR, qb, width)), bf((parts, qb, width)), bf((total, width)),
            fl((parts, qb, LANE)), fl((parts, NEAR, qb, LANE)),
            bf((total, wide)), bf((parts, hb, wide)), bf((parts, qb, wide)), bf((parts, qb, wide)),
            fl((total, LANE)), fl((parts, hb, LANE)), fl((parts, qb, LANE)), fl((parts, qb, LANE)),
            bf((total, top * ff)), bf((total, width)), bf((parts, NEAR, qb, width)),
            dma((NEAR,)),
        ] + [dma(n) for n in sems],
        compiler_params=pltpu.CompilerParams(collective_id=1, has_side_effects=True, vmem_limit_bytes=60 * MIB),
        cost_estimate=pl.CostEstimate(flops=6 * total * width * experts * ff, bytes_accessed=12 * MIB, transcendentals=0),
    )(mixed, wo, x_in, gain, w_router, chosen, w_act, w_lin, w_down.reshape(experts * ff, width))


def solution(mesh):
    x_count = mesh.shape['x']
    cache_spec = P('dp', None, 'y', None)
    in_specs = (P(None, 'dp'), P('dp'), P(None, 'dp', None), P(None, 'x'), cache_spec, cache_spec, P('x'), P('x', 'y'), P('x', 'y'), P('x', 'y'), P('y', 'x'), P('x'), P('x', None), P(None, 'x', 'y'), P(None, 'x', 'y'), P(None, 'y', 'x'))
    out_specs = (P(None, 'dp', 'x'), cache_spec, cache_spec)

    def per_device(tokens, lengths, choices, emb_table, k_cache, v_cache, g_attn, w_q, w_k, w_v, w_o, g_ffn, w_router, w_act, w_lin, w_down):
        steps, nb = tokens.shape
        seq, kvl, hdim = k_cache.shape[1:]
        q_cols, kv_cols = w_q.shape[1], w_k.shape[1]
        width = emb_table.shape[1]
        width_full = width * x_count
        group = q_cols // kv_cols
        rows = steps * nb
        x_in = emb_table.at[tokens].get(mode="promise_in_bounds", wrap_negative_indices=False).reshape(rows, width)
        line = lax.broadcasted_iota(jnp.int32, (3, width), 0)
        spread = jnp.pad(lengths.astype(F32), (0, width - nb))
        gains = jnp.where(line == 0, g_attn.astype(F32)[None, :], jnp.where(line == 1, g_ffn.astype(F32)[None, :], spread[None, :]))
        proj = front(x_in, gains, w_q, w_k, w_v, steps, width_full)
        kc = k_cache.transpose(0, 2, 3, 1).reshape(nb, kv_cols, seq)
        vc = v_cache.transpose(0, 2, 3, 1).reshape(nb, kv_cols, seq)
        mixed, ko, vo = attention(lengths, proj, kc, vc, group)
        hidden = tail(mixed, w_o, x_in, gains, w_router.T, choices.transpose(0, 2, 1), w_act, w_lin, w_down, width_full).reshape(steps, nb, width)
        ko = ko.reshape(nb, kvl, hdim, seq).transpose(0, 3, 1, 2)
        vo = vo.reshape(nb, kvl, hdim, seq).transpose(0, 3, 1, 2)
        return hidden, ko, vo

    return jax.shard_map(per_device, mesh=mesh, in_specs=in_specs, out_specs=out_specs, check_vma=False)
```
